16 devices in a mesh: rep: 2 (over y, z), dp: 8 (over x, core).
Axes of the slice: x: 4, y: 2, z: 1, core: 2. Of those that a mesh axis runs over, the one named last changes fastest.
The devices are a block of a 4x4x8 slice.
Arguments:
- x: bfloat16 [16, 2048, 896], P(('rep', 'dp')), parts along dimension 0
- dy: bfloat16 [16, 2048, 896], P(('rep', 'dp')), parts along dimension 0
- w_gate: bfloat16 [2, 896, 2304], replicated
- w_up: bfloat16 [2, 896, 2304], replicated
- w_down: bfloat16 [2, 2304, 896], replicated
- m_w_gate: float32 [2, 896, 2304], P(None, 'dp')
- m_w_up: float32 [2, 896, 2304], P(None, 'dp')
- m_w_down: float32 [2, 2304, 896], P(None, 'dp')
- v_w_gate: float32 [2, 896, 2304], P(None, 'dp')
- v_w_up: float32 [2, 896, 2304], P(None, 'dp')
- v_w_down: float32 [2, 2304, 896], P(None, 'dp')
Outputs:
- output 1: bfloat16 [4, 896, 2304], P('rep'), parts along dimension 0
- output 2: bfloat16 [4, 896, 2304], P('rep'), parts along dimension 0
- output 3: bfloat16 [4, 2304, 896], P('rep'), parts along dimension 0
- output 4: float32 [4, 896, 2304], P('rep', 'dp'), parts along dimension 0
- output 5: float32 [4, 896, 2304], P('rep', 'dp'), parts along dimension 0
- output 6: float32 [4, 2304, 896], P('rep', 'dp'), parts along dimension 0
- output 7: float32 [4, 896, 2304], P('rep', 'dp'), parts along dimension 0
- output 8: float32 [4, 896, 2304], P('rep', 'dp'), parts along dimension 0
- output 9: float32 [4, 2304, 896], P('rep', 'dp'), parts along dimension 0
There are 2 independent parts. The reference program is written for one: setup_inputs(seed, part) draws one part's arguments, and reference() takes and returns one part's arrays. A program takes and returns all parts, laid end to end along the dimension named above; an argument that names none is the same for every part.
All inputs are finite; a program needn't handle non-finite values.
Results may differ from the reference program's by a relative error of at most 0.022.
Values are sent between devices in bfloat16 or wider.
A program may use at most 768 MiB of HBM per device.

```python
import jax
import jax.numpy as jnp
from jax import lax

SEQUENCES = 8
TOKENS = 2048
D = 896
FF = 2304
LAYERS = 2
NAMES = ("w_gate", "w_up", "w_down")
SHAPES = {"w_gate": (LAYERS, D, FF), "w_up": (LAYERS, D, FF), "w_down": (LAYERS, FF, D)}


def bump(key, n, height):
    away = (jnp.arange(n, dtype=jnp.int32) - jax.random.randint(key, (), 0, n, jnp.int32)) % n
    return jnp.where(away < n // 8, height, 1.0)


def together(key, own, strength):
    shared = jax.random.normal(key, own.shape[1:], jnp.float32)
    return (own + strength * shared) * lax.rsqrt(1 + strength * strength)


def setup_inputs(seed: int = 0, part: int = 0) -> dict:
    kx, kdy, ka, kb, kz, kf, kh, kl, *keys = jax.random.split(jax.random.key(seed), 8 + 3 * len(NAMES))
    kx, kdy, ka, kb = (jax.random.fold_in(k, part) for k in (kx, kdy, ka, kb))
    kw, km, kv = (keys[i::3] for i in range(3))
    shape = (SEQUENCES, TOKENS, D)
    much_x, much_dy = jax.random.uniform(kz, (2,), jnp.float32, 0.0, 1.0)
    loud = 2.0 ** jax.random.uniform(jax.random.fold_in(kz, 1), (), jnp.float32, -1.0, 2.0)
    layers = 2.0 ** jax.random.uniform(kl, (LAYERS, 1, 1), jnp.float32, -1.0, 1.0)
    x = together(ka, jax.random.normal(kx, shape, jnp.float32), much_x) * bump(kf, D, 4.0)
    dy = together(kb, jax.random.normal(kdy, shape, jnp.float32), much_dy)
    drawn = {"x": x.astype(jnp.bfloat16), "dy": (loud * dy * (SEQUENCES * TOKENS) ** -0.5).astype(jnp.bfloat16)}
    for key, name in zip(kw, NAMES, strict=True):
        w = jax.random.normal(key, SHAPES[name], jnp.float32) * SHAPES[name][1] ** -0.5
        drawn[name] = (w * {"w_gate": 1.0, "w_up": bump(kh, FF, 4.0), "w_down": layers}[name]).astype(jnp.bfloat16)
    for key, name in zip(km, NAMES, strict=True):
        drawn[f"m_{name}"] = 0.1 * jax.random.normal(key, SHAPES[name], jnp.float32)
    for key, name in zip(kv, NAMES, strict=True):
        drawn[f"v_{name}"] = jax.random.uniform(key, SHAPES[name], jnp.float32, 0.005, 0.015)
    return drawn


def matmul(a, w):
    return jnp.dot(a, w, preferred_element_type=jnp.float32).astype(jnp.bfloat16)


def normed(h):
    wide = h.astype(jnp.float32)
    scale = lax.rsqrt(jnp.mean(wide**2, -1, keepdims=True) + 1e-6)
    return (wide * scale).astype(jnp.bfloat16)


def layer(h, w):
    a = normed(h)
    gate = jnp.dot(a, w["w_gate"], preferred_element_type=jnp.float32)
    up = jnp.dot(a, w["w_up"], preferred_element_type=jnp.float32)
    return h + matmul((jax.nn.silu(gate) * up).astype(jnp.bfloat16), w["w_down"])


def adamw(w, m, v, g):
    m = 0.9 * m + 0.1 * g
    v = 0.95 * v + 0.05 * g * g
    step = m * lax.rsqrt(v + 1e-8) + 0.1 * w
    return (w - 0.02 * step).astype(jnp.bfloat16), m, v


def clipped(gradients, sum_of_squares, count):
    factor = jnp.minimum(1.0, 0.5 * lax.rsqrt(sum_of_squares / count + 1e-30))
    return [g * factor for g in gradients]


def stack(weights, h):
    return lax.scan(lambda h, w: (layer(h, w), None), h, weights)[0]


def reference(x, dy, w_gate, w_up, w_down, m_w_gate, m_w_up, m_w_down, v_w_gate, v_w_up, v_w_down):
    weights = dict(zip(NAMES, (w_gate, w_up, w_down), strict=True))

    def take(so_far, sequence):
        h, by_y = sequence
        _, back = jax.vjp(lambda w: stack(w, h), weights)
        return jax.tree.map(lambda total, term: total + term.astype(jnp.float32), so_far, back(by_y)[0]), None

    none_yet = {name: jnp.zeros(w.shape, jnp.float32) for name, w in weights.items()}
    by_weights, _ = lax.scan(take, none_yet, (x, dy))
    gradients = [by_weights[name].astype(jnp.bfloat16).astype(jnp.float32) for name in NAMES]
    gradients = clipped(gradients, sum(jnp.sum(g * g) for g in gradients), sum(g.size for g in gradients))
    new = [
        adamw(w.astype(jnp.float32), m, v, g)
        for w, m, v, g in zip((w_gate, w_up, w_down), (m_w_gate, m_w_up, m_w_down), (v_w_gate, v_w_up, v_w_down), gradients, strict=True)
    ]
    return tuple(one[which] for which in range(3) for one in new)
```

```python
import functools

import jax
import jax.numpy as jnp
from jax import lax
from jax.experimental import pallas as pl
from jax.experimental.pallas import tpu as pltpu
from jax.sharding import PartitionSpec as P

F32, BF16 = jnp.float32, jnp.bfloat16
NT = (((1,), (1,)), ((), ()))

def dot(a, b):
    return jnp.dot(a, b, preferred_element_type=F32)
def dot_t(a, b):
    return lax.dot_general(a, b, NT, preferred_element_type=F32)

def norm_of(h):
    wide = h.astype(F32)
    scale = lax.rsqrt(jnp.mean(wide * wide, -1, keepdims=True) + 1e-6)
    return wide, scale

def tokens_kernel(nf, x_ref, dy_ref, wg_hbm, wu_hbm, wd_hbm, s_ref, a_ref, dh_ref, wg, wu, wd, g0, u0, sems):
    i = pl.program_id(0)
    ff = wg.shape[2]
    fb = ff // nf
    cols = [slice(k * fb, (k + 1) * fb) for k in range(nf)]
    hbm, vm = (wg_hbm, wu_hbm, wd_hbm), (wg, wu, wd)
    def copies(l):
        return [pltpu.make_async_copy(h.at[l], v.at[l], sems.at[l, j]) for j, (h, v) in enumerate(zip(hbm, vm))]
    @pl.when(i == 0)
    def _():
        for l in range(2):
            for c in copies(l): c.start()
    def arrive(l, j):
        @pl.when(i == 0)
        def _(): copies(l)[j].wait()

    x = x_ref[0]
    wide, scale = norm_of(x)
    a0 = (wide * scale).astype(BF16)
    a_ref[1] = a0
    arrive(0, 0); arrive(0, 1); arrive(0, 2)
    down = None
    for c in cols:
        g = dot(a0, wg[0, :, c]); u = dot(a0, wu[0, :, c])
        g0[:, c] = g; u0[:, c] = u
        p = (g * jax.nn.sigmoid(g) * u).astype(BF16)
        s_ref[5, :, c] = p
        d = dot(p, wd[0, c, :])
        down = d if down is None else down + d
    h1 = x + down.astype(BF16)
    wide1, scale1 = norm_of(h1)
    a1 = (wide1 * scale1).astype(BF16)
    a_ref[0] = a1
    dy = dy_ref[0]
    dh_ref[0] = dy
    arrive(1, 0); arrive(1, 1); arrive(1, 2)
    dag = dau = None
    for c in cols:
        g = dot(a1, wg[1, :, c]); u = dot(a1, wu[1, :, c])
        dp = dot_t(dy, wd[1, c, :]).astype(BF16).astype(F32)
        sig = jax.nn.sigmoid(g); si = g * sig
        s_ref[2, :, c] = (si * u).astype(BF16)
        dg = (dp * u * (sig + si * (1 - sig))).astype(BF16)
        du = (dp * si).astype(BF16)
        s_ref[0, :, c] = dg
        s_ref[1, :, c] = du
        e = dot_t(dg, wg[1, :, c]); f = dot_t(du, wu[1, :, c])
        dag = e if dag is None else dag + e
        dau = f if dau is None else dau + f
    da = (dag.astype(BF16) + dau.astype(BF16)).astype(F32)
    coef = jnp.sum(da * wide1, -1, keepdims=True) * (scale1 * scale1 * scale1) * (-1.0 / da.shape[-1])
    dh1 = dy + (da * scale1 + wide1 * coef).astype(BF16)
    dh_ref[1] = dh1
    for c in cols:
        dp = dot_t(dh1, wd[0, c, :]).astype(BF16).astype(F32)
        g = g0[:, c]; u = u0[:, c]
        sig = jax.nn.sigmoid(g); si = g * sig
        s_ref[3, :, c] = (dp * u * (sig + si * (1 - sig))).astype(BF16)
        s_ref[4, :, c] = (dp * si).astype(BF16)

def tokens(x, dy, wg, wu, wd, tm=256, nf=3):
    _, t, d = x.shape
    ff = wg.shape[2]
    tile = pl.BlockSpec((1, tm, d), lambda i: (0, i, 0))
    anyspec = pl.BlockSpec(memory_space=pl.ANY)
    return pl.pallas_call(
        functools.partial(tokens_kernel, nf), grid=(t // tm,),
        in_specs=[tile, tile, anyspec, anyspec, anyspec],
        out_specs=[pl.BlockSpec((6, tm, ff), lambda i: (0, i, 0)), pl.BlockSpec((2, tm, d), lambda i: (0, i, 0)), pl.BlockSpec((2, tm, d), lambda i: (0, i, 0))],
        out_shape=[jax.ShapeDtypeStruct((6, t, ff), BF16), jax.ShapeDtypeStruct((2, t, d), BF16), jax.ShapeDtypeStruct((2, t, d), BF16)],
        scratch_shapes=[pltpu.VMEM(wg.shape, BF16), pltpu.VMEM(wu.shape, BF16), pltpu.VMEM(wd.shape, BF16),
                        pltpu.VMEM((tm, ff), F32), pltpu.VMEM((tm, ff), F32), pltpu.SemaphoreType.DMA((2, 3))],
        compiler_params=pltpu.CompilerParams(vmem_limit_bytes=67043328, dimension_semantics=("arbitrary",)),
        name="tokens",
    )(x, dy, wg, wu, wd)


def adamw(w, m, v, g):
    m = 0.9 * m + 0.1 * g
    v = 0.95 * v + 0.05 * g * g
    step = m * lax.rsqrt(v + 1e-8) + 0.1 * w
    return (w - 0.02 * step).astype(BF16), m, v


def solution(mesh):
    n = mesh.shape["dp"]

    def step(x, dy, wg, wu, wd, mg, mu, md, vg, vu, vd):
        s, a, dh = tokens(x, dy, wg, wu, wd)

        def grad(lhs, rhs):
            term = lax.dot_general(lhs, rhs, (((0,), (0,)), ((), ())), preferred_element_type=F32).astype(BF16)
            return lax.psum_scatter(term, "dp", scatter_dimension=0, tiled=True).astype(F32)

        first, last = {}, {}
        for to, l in ((last, 0), (first, 1)):
            to["g"] = grad(a[l], s[3 * l])
            to["u"] = grad(a[l], s[3 * l + 1])
            to["d"] = grad(s[3 * l + 2], dh[l])
        grads = [jnp.stack([first[k], last[k]]) for k in "gud"]
        count = n * sum(g.size for g in grads)
        total = lax.psum(sum(jnp.sum(g * g) for g in grads), "dp")
        factor = jnp.minimum(1.0, 0.5 * lax.rsqrt(total / count + 1e-30))
        me = lax.axis_index("dp")
        new = []
        for w, m, v, g in zip((wg, wu, wd), (mg, mu, md), (vg, vu, vd), grads):
            rows = m.shape[1]
            own = lax.dynamic_slice_in_dim(w, me * rows, rows, 1).astype(F32)
            nw, nm, nv = adamw(own, m, v, g * factor)
            new.append((lax.all_gather(nw, "dp", axis=1, tiled=True), nm, nv))
        return tuple(one[i] for i in range(3) for one in new)

    data, whole, rows = P(("rep", "dp"), None, None), P(None, None, None), P(None, "dp", None)
    return jax.shard_map(step, mesh=mesh, in_specs=(data,) * 2 + (whole,) * 3 + (rows,) * 6,
                         out_specs=(P("rep", None, None),) * 3 + (P("rep", "dp", None),) * 6, check_vma=False)
```

```python
import functools

import jax
import jax.numpy as jnp
from jax import lax
from jax.experimental import pallas as pl
from jax.experimental.pallas import tpu as pltpu
from jax.sharding import PartitionSpec as P

F32, BF16 = jnp.float32, jnp.bfloat16
NT = (((1,), (1,)), ((), ()))

def dot(a, b):
    return jnp.dot(a, b, preferred_element_type=F32)
def dot_t(a, b):
    return lax.dot_general(a, b, NT, preferred_element_type=F32)

def norm_of(h):
    wide = h.astype(F32)
    scale = lax.rsqrt(jnp.mean(wide * wide, -1, keepdims=True) + 1e-6)
    return wide, scale

def tokens_kernel(nf, x_ref, dy_ref, wg_hbm, wu_hbm, wd_hbm, s_ref, a_ref, dh_ref, wg, wu, wd, g0, u0, sems):
    i = pl.program_id(0)
    ff = wg.shape[2]
    fb = ff // nf
    cols = [slice(k * fb, (k + 1) * fb) for k in range(nf)]
    hbm, vm = (wg_hbm, wu_hbm, wd_hbm), (wg, wu, wd)
    def copies(l):
        return [pltpu.make_async_copy(h.at[l], v.at[l], sems.at[l, j]) for j, (h, v) in enumerate(zip(hbm, vm))]
    @pl.when(i == 0)
    def _():
        for l in range(2):
            for c in copies(l): c.start()
    def arrive(l, j):
        @pl.when(i == 0)
        def _(): copies(l)[j].wait()

    x = x_ref[0]
    wide, scale = norm_of(x)
    a0 = (wide * scale).astype(BF16)
    a_ref[1] = a0.T
    arrive(0, 0); arrive(0, 1); arrive(0, 2)
    down = None
    for c in cols:
        g = dot(a0, wg[0, :, c]); u = dot(a0, wu[0, :, c])
        g0[:, c] = g; u0[:, c] = u
        p = (g * jax.nn.sigmoid(g) * u).astype(BF16)
        s_ref[5, :, c] = p
        d = dot(p, wd[0, c, :])
        down = d if down is None else down + d
    h1 = x + down.astype(BF16)
    wide1, scale1 = norm_of(h1)
    a1 = (wide1 * scale1).astype(BF16)
    a_ref[0] = a1.T
    dy = dy_ref[0]
    dh_ref[0] = dy
    arrive(1, 0); arrive(1, 1); arrive(1, 2)
    dag = dau = None
    for c in cols:
        g = dot(a1, wg[1, :, c]); u = dot(a1, wu[1, :, c])
        dp = dot_t(dy, wd[1, c, :]).astype(BF16).astype(F32)
        sig = jax.nn.sigmoid(g); si = g * sig
        s_ref[2, :, c] = (si * u).astype(BF16)
        dg = (dp * u * (sig + si * (1 - sig))).astype(BF16)
        du = (dp * si).astype(BF16)
        s_ref[0, :, c] = dg
        s_ref[1, :, c] = du
        e = dot_t(dg, wg[1, :, c]); f = dot_t(du, wu[1, :, c])
        dag = e if dag is None else dag + e
        dau = f if dau is None else dau + f
    da = (dag.astype(BF16) + dau.astype(BF16)).astype(F32)
    coef = jnp.sum(da * wide1, -1, keepdims=True) * (scale1 * scale1 * scale1) * (-1.0 / da.shape[-1])
    dh1 = dy + (da * scale1 + wide1 * coef).astype(BF16)
    dh_ref[1] = dh1
    for c in cols:
        dp = dot_t(dh1, wd[0, c, :]).astype(BF16).astype(F32)
        g = g0[:, c]; u = u0[:, c]
        sig = jax.nn.sigmoid(g); si = g * sig
        s_ref[3, :, c] = (dp * u * (sig + si * (1 - sig))).astype(BF16)
        s_ref[4, :, c] = (dp * si).astype(BF16)

def tokens(x, dy, wg, wu, wd, tm=256, nf=3):
    _, t, d = x.shape
    ff = wg.shape[2]
    tile = pl.BlockSpec((1, tm, d), lambda i: (0, i, 0))
    anyspec = pl.BlockSpec(memory_space=pl.ANY)
    return pl.pallas_call(
        functools.partial(tokens_kernel, nf), grid=(t // tm,),
        in_specs=[tile, tile, anyspec, anyspec, anyspec],
        out_specs=[pl.BlockSpec((6, tm, ff), lambda i: (0, i, 0)), pl.BlockSpec((2, d, tm), lambda i: (0, 0, i)), pl.BlockSpec((2, tm, d), lambda i: (0, i, 0))],
        out_shape=[jax.ShapeDtypeStruct((6, t, ff), BF16), jax.ShapeDtypeStruct((2, d, t), BF16), jax.ShapeDtypeStruct((2, t, d), BF16)],
        scratch_shapes=[pltpu.VMEM(wg.shape, BF16), pltpu.VMEM(wu.shape, BF16), pltpu.VMEM(wd.shape, BF16),
                        pltpu.VMEM((tm, ff), F32), pltpu.VMEM((tm, ff), F32), pltpu.SemaphoreType.DMA((2, 3))],
        compiler_params=pltpu.CompilerParams(vmem_limit_bytes=67043328, dimension_semantics=("arbitrary",)),
        name="tokens",
    )(x, dy, wg, wu, wd)
TN = (((0,), (0,)), ((), ()))
NK = 3
RING = 11

def grads_kernel(n, s_hbm, at_hbm, dh_hbm, g_ref, ss_ref, at, dh, inb, st, re, sb, rt, cb, rf, ss, ssr,
                 in_sem, ld_sem, e_s, e_r, r1_s, r1_r, r2_s, r2_r, x_s, x_r):
    me = lax.axis_index("dp")
    core, chip = lax.rem(me, 2), lax.div(me, 2)
    chips = n // 2
    mats, t, ff = s_hbm.shape
    d = at_hbm.shape[1]
    chunks = mats * NK
    cw, rg, rk = ff // NK, d // n, ff // n // NK
    rows = g_ref.shape[1]
    half = rows // 2
    A, B = pl.ds(0, half), pl.ds(half, half)
    nxt, prv, far = lax.rem(chip + 1, chips), lax.rem(chip + chips - 1, chips), lax.rem(chip + 2, chips)
    right, left, partner = nxt * 2 + core, prv * 2 + core, chip * 2 + (1 - core)

    def remote(src, dst, send, recv, to):
        return pltpu.make_async_remote_copy(src_ref=src, dst_ref=dst, send_sem=send, recv_sem=recv,
                                            device_id={"dp": to}, device_id_type=pl.DeviceIdType.MESH)

    def fetch(c):
        return pltpu.make_async_copy(s_hbm.at[lax.div(c, NK), :, pl.ds(pl.multiple_of(lax.rem(c, NK) * cw, cw), cw)],
                                     inb.at[lax.rem(c, 2)], in_sem.at[lax.rem(c, 2)])

    def loads(l):
        return (pltpu.make_async_copy(at_hbm.at[l], at, ld_sem.at[0]), pltpu.make_async_copy(dh_hbm.at[l], dh, ld_sem.at[1]))

    fetch(0).start()
    barrier = pltpu.get_barrier_semaphore()
    for o in range(1, n):
        pl.semaphore_signal(barrier, inc=1, device_id={"dp": lax.rem(me + o, n)}, device_id_type=pl.DeviceIdType.MESH)
    pl.semaphore_wait(barrier, n - 1)
    ss[...] = jnp.zeros_like(ss)

    def compute(c, _):
        mat, k = lax.div(c, NK), lax.rem(c, NK)
        layer, kind = lax.div(mat, 3), lax.rem(mat, 3)
        fresh = lax.rem(c, 3 * NK) == 0

        @pl.when(fresh)
        def _():
            for one in loads(layer):
                one.start()
        fetch(c).wait()

        @pl.when(c + 1 < chunks)
        def _():
            fetch(c + 1).start()

        @pl.when(fresh)
        def _():
            for one in loads(layer):
                one.wait()
        slot = lax.rem(c, 2)

        @pl.when(kind < 2)
        def _():
            def sub(j, _):
                out = jnp.dot(at[...], inb[slot, :, pl.ds(pl.multiple_of(j * 256, 256), 256)], preferred_element_type=F32).astype(BF16)
                for b in range(n):
                    for i in range(2):
                        st[lax.rem(core + b, 2), lax.rem(c, RING), b // 2, pl.ds(pl.multiple_of((2 * j + i) * rg, 16), rg), :] = \
                            out[b * rg:(b + 1) * rg, i * 128:(i + 1) * 128]
                return 0
            lax.fori_loop(0, cw // 256, sub, 0)

        @pl.when(kind == 2)
        def _():
            def sub(j, _):
                wide = cw // 2
                out = lax.dot_general(inb[slot, :, pl.ds(pl.multiple_of(j * wide, 128), wide)], dh[...], TN, preferred_element_type=F32).astype(BF16)
                for i in range(wide // rk):
                    q = (2 * k + j) * (wide // rk) + i
                    b, part = lax.div(q, NK), lax.rem(q, NK)
                    for tile in range(d // 128):
                        st[lax.rem(core + b, 2), lax.rem(mat * NK + part, RING), lax.div(b, 2), tile * rk:(tile + 1) * rk, :] = \
                            out[i * rk:(i + 1) * rk, tile * 128:(tile + 1) * 128]
                return 0
            lax.fori_loop(0, 2, sub, 0)
        return 0

    def exchange(c):
        return remote(st.at[1, lax.rem(c, RING)], re.at[c], e_s.at[lax.rem(c, 4)], e_r.at[c], partner)

    def first(c):
        r, q = lax.rem(c, 3), lax.rem(c, 4)
        return (remote(sb.at[r, 0], rt.at[c, 0], r1_s.at[q, 0], r1_r.at[c, 0], left),
                remote(sb.at[r, 1], rt.at[c, 1], r1_s.at[q, 1], r1_r.at[c, 1], right),
                remote(sb.at[r, 2], rf.at[c, 0, B], r1_s.at[q, 2], r1_r.at[c, 2], left),
                remote(sb.at[r, 3], rf.at[c, 1, A], r1_s.at[q, 3], r1_r.at[c, 3], right))

    def second(c):
        r, q = lax.rem(c, 3), lax.rem(c, 4)
        return (remote(cb.at[r, 0], rf.at[c, 0, A], r2_s.at[q, 0], r2_r.at[c, 0], left),
                remote(cb.at[r, 1], rf.at[c, 1, B], r2_s.at[q, 1], r2_r.at[c, 1], right))

    def pair(c, to, part):
        return st[0, lax.rem(c, RING), to, part, :].astype(F32) + re[c, to, part, :].astype(F32)

    def step(s, _):
        def done(u):
            ahead = jnp.where(u >= 5, 1, 0) + jnp.where(u >= 6, 1, 0)
            return jnp.minimum(u + 1 + ahead, chunks)
        lax.fori_loop(jnp.where(s == 0, 0, done(s - 1)), done(s), compute, 0)

        @pl.when((s >= 2) & (s < chunks + 2))
        def _():
            c = s - 2
            exchange(c).wait()
            r = lax.rem(c, 3)
            sb[r, 0] = pair(c, far, A).astype(BF16)
            sb[r, 1] = pair(c, far, B).astype(BF16)
            sb[r, 2] = pair(c, prv, B).astype(BF16)
            sb[r, 3] = pair(c, nxt, A).astype(BF16)

        @pl.when((s >= 4) & (s < chunks + 4))
        def _():
            c = s - 4
            for i, one in enumerate(first(c)):
                one.wait_send()
                if i < 2:
                    one.wait_recv()
            r = lax.rem(c, 3)
            cb[r, 0] = (pair(c, prv, A) + rt[c, 0].astype(F32)).astype(BF16)
            cb[r, 1] = (pair(c, nxt, B) + rt[c, 1].astype(F32)).astype(BF16)

        @pl.when(s < chunks)
        def _():
            exchange(s).start()

        @pl.when((s >= 4) & (s < chunks + 4))
        def _():
            for one in second(s - 4):
                one.start()

        @pl.when((s >= 2) & (s < chunks + 2))
        def _():
            for one in first(s - 2):
                one.start()

        @pl.when(s >= 6)
        def _():
            c = s - 6
            for one in first(c)[2:]:
                one.wait_recv()
            for one in second(c):
                one.wait()
            g = (pair(c, chip, pl.ds(0, rows)) + rf[c, 0].astype(F32) + rf[c, 1].astype(F32)).astype(BF16)
            g_ref[c] = g
            wide = g.astype(F32)
            ss[...] += jnp.sum((wide * wide).reshape(rows // 8, 8, 128), 0)
        return 0

    lax.fori_loop(0, chunks + 6, step, 0)
    tell = [remote(ss, ssr.at[o], x_s.at[o], x_r.at[o], lax.rem(me + o, n)) for o in range(1, n)]
    for one in tell:
        one.start()
    total = ss[...]
    for o, one in enumerate(tell, 1):
        one.wait()
        total = total + ssr[o]
    ss_ref[...] = total

def grads(n, s, at, dh):
    mats, t, ff = s.shape
    d = at.shape[1]
    chunks, rows = mats * NK, ff // NK // 128 * (d // n)
    assert rows == d // 128 * (ff // n // NK)
    half, dma = rows // 2, pltpu.SemaphoreType.DMA
    anyspec = pl.BlockSpec(memory_space=pl.ANY)
    return pl.pallas_call(
        functools.partial(grads_kernel, n),
        in_specs=[anyspec] * 3,
        out_specs=[pl.BlockSpec(memory_space=pltpu.VMEM)] * 2,
        out_shape=[jax.ShapeDtypeStruct((chunks, rows, 128), BF16), jax.ShapeDtypeStruct((8, 128), F32)],
        scratch_shapes=[pltpu.VMEM((d, t), BF16), pltpu.VMEM((t, d), BF16), pltpu.VMEM((2, t, ff // NK), BF16),
                        pltpu.VMEM((2, RING, n // 2, rows, 128), BF16), pltpu.VMEM((chunks, n // 2, rows, 128), BF16),
                        pltpu.VMEM((3, 4, half, 128), BF16), pltpu.VMEM((chunks, 2, half, 128), BF16),
                        pltpu.VMEM((3, 2, half, 128), BF16), pltpu.VMEM((chunks, 2, rows, 128), BF16),
                        pltpu.VMEM((8, 128), F32), pltpu.VMEM((n, 8, 128), F32),
                        dma((2,)), dma((2,)), dma((4,)), dma((chunks,)), dma((4, 4)), dma((chunks, 4)), dma((4, 2)), dma((chunks, 2)),
                        dma((n,)), dma((n,))],
        compiler_params=pltpu.CompilerParams(vmem_limit_bytes=67043328, collective_id=0, has_side_effects=True),
        name="grads",
    )(s, at, dh)

def adam_kernel(count, me_ref, ss_ref, g_ref, *refs):
    ws, ms, vs, outs = refs[:3], refs[3:6], refs[6:9], refs[9:]
    total = jnp.sum(ss_ref[...], keepdims=True)
    factor = jnp.minimum(1.0, 0.5 * lax.rsqrt(total / count + 1e-30))
    for i in range(3):
        rows, cols = ms[i].shape[1:]
        for t in range(cols // 128):
            c = slice(t * 128, (t + 1) * 128)
            g = g_ref[0, i, 0, t * rows:(t + 1) * rows, :].astype(F32) * factor
            m = 0.9 * ms[i][0, :, c] + 0.1 * g
            v = 0.95 * vs[i][0, :, c] + 0.05 * g * g
            w = ws[i][0, :, c].astype(F32)
            outs[i][0, :, c] = (w - 0.02 * (m * lax.rsqrt(v + 1e-8) + 0.1 * w)).astype(BF16)
            outs[3 + i][0, :, c] = m
            outs[6 + i][0, :, c] = v

def adam(n, me, ss, g, ws, ms, vs):
    layers, d, ff = ws[0].shape
    rg, rk, cw = d // n, ff // n // NK, ff // NK
    wide = lambda at: pl.BlockSpec((1, rg, cw), lambda l, k, me: (l, at(me), k))
    tall = lambda at: pl.BlockSpec((1, rk, d), lambda l, k, me: (l, NK * at(me) + k, 0))
    none, mine = (lambda me: 0), (lambda me: me[0])
    three = lambda at: [wide(at), wide(at), tall(at)]
    shapes = lambda dt: [jax.ShapeDtypeStruct(m.shape, dt) for m in ms]
    grid = pltpu.PrefetchScalarGridSpec(
        num_scalar_prefetch=1, grid=(layers, NK),
        in_specs=[pl.BlockSpec((8, 128), lambda l, k, me: (0, 0)),
                  pl.BlockSpec((1, 3, 1) + g.shape[1:], lambda l, k, me: (layers - 1 - l, 0, k, 0, 0))]
        + three(mine) + three(none) * 2,
        out_specs=three(none) * 3)
    count = n * sum(m.size for m in ms)
    out = pl.pallas_call(functools.partial(adam_kernel, count), grid_spec=grid, out_shape=shapes(BF16) + shapes(F32) * 2,
                         compiler_params=pltpu.CompilerParams(vmem_limit_bytes=40 << 20), name="adam",
                         )(me, ss, g.reshape((layers, 3, NK) + g.shape[1:]), *ws, *ms, *vs)
    return out[:3], out[3:6], out[6:]

def gather_kernel(n, *refs):
    mine, outs, (in_sem, s_sem, r_sem) = refs[:3], refs[3:6], refs[6:]
    me = lax.axis_index("dp")
    chips = n // 2
    core, chip = lax.rem(me, 2), lax.div(me, 2)
    owner = lambda c, q=None: lax.rem(c + chips, chips) * 2 + (core if q is None else q)
    right, left, partner = owner(chip + 1), owner(chip - 1), owner(chip, 1 - core)
    pieces = [(i, l) for l in range(2) for i in range(3)]

    def place(i, l, b):
        rows = mine[i].shape[1]
        return outs[i].at[l, pl.ds(pl.multiple_of(b * rows, 16), rows), :]
    own = [pltpu.make_async_copy(mine[i].at[l], place(i, l, me), in_sem.at[p]) for p, (i, l) in enumerate(pieces)]
    for one in own:
        one.start()
    barrier = pltpu.get_barrier_semaphore()
    for to in (left, right, partner):
        pl.semaphore_signal(barrier, inc=1, device_id={"dp": to}, device_id_type=pl.DeviceIdType.MESH)
    pl.semaphore_wait(barrier, 3)
    for one in own:
        one.wait()

    def copy(kind, p, there=False):
        i, l = pieces[p]
        far_right = l == 0
        if kind == 0:
            to, b = right, me
        elif kind == 1:
            to, b = left, me
        elif kind == 2:
            to, b = (right, owner(chip - 1)) if far_right else (left, owner(chip + 1))
        else:
            to = partner
            b = (me, owner(chip - 1), owner(chip + 1), owner(chip + 2))[kind - 3]
        ref = place(i, l, b)
        return pltpu.make_async_remote_copy(src_ref=ref, dst_ref=ref, send_sem=s_sem.at[kind, p], recv_sem=r_sem.at[kind, p],
                                            device_id={"dp": to}, device_id_type=pl.DeviceIdType.MESH)
    zero, one_ = [p for p, (i, l) in enumerate(pieces) if l == 0], [p for p, (i, l) in enumerate(pieces) if l == 1]
    for a, b in zip(zero + one_, one_ + zero):
        copy(0, a).start()
        copy(1, b).start()
    for p in range(len(pieces)):
        copy(3, p).start()
    for a, b in zip(zero, one_):
        copy(0, a).wait_recv()
        copy(2, a).start()
        copy(4, a).start()
        copy(1, b).wait_recv()
        copy(2, b).start()
        copy(5, b).start()
    for a, b in zip(one_, zero):
        copy(0, a).wait_recv()
        copy(4, a).start()
        copy(1, b).wait_recv()
        copy(5, b).start()
    for a, b in zip(zero, one_):
        for p in (a, b):
            copy(2, p).wait_recv()
            copy(6, p).start()
    for p in range(len(pieces)):
        for kind in range(7):
            copy(kind, p).wait_send()
            if kind >= 3:
                copy(kind, p).wait_recv()

def gather(n, news):
    dma = pltpu.SemaphoreType.DMA
    full = [(w.shape[0], n * w.shape[1], w.shape[2]) for w in news]
    return pl.pallas_call(
        functools.partial(gather_kernel, n),
        in_specs=[pl.BlockSpec(memory_space=pl.ANY)] * 3,
        out_specs=[pl.BlockSpec(memory_space=pltpu.VMEM)] * 3,
        out_shape=[pltpu.VMEM(s, BF16) for s in full],
        scratch_shapes=[dma((6,)), dma((7, 6)), dma((7, 6))],
        compiler_params=pltpu.CompilerParams(vmem_limit_bytes=1 << 20, collective_id=1, has_side_effects=True),
        name="gather",
    )(*news)

def store_kernel(*refs):
    half = (len(refs) - 1) // 2
    copies = [pltpu.make_async_copy(refs[i], refs[half + i], refs[-1].at[i]) for i in range(half)]
    for one in copies:
        one.start()
    for one in copies:
        one.wait()

def store(arrays):
    k = len(arrays)
    return pl.pallas_call(
        store_kernel, in_specs=[pl.BlockSpec(memory_space=pltpu.VMEM)] * k, out_specs=[pl.BlockSpec(memory_space=pltpu.HBM)] * k,
        out_shape=[pltpu.HBM(a.shape, a.dtype) for a in arrays], scratch_shapes=[pltpu.SemaphoreType.DMA((k,))],
        compiler_params=pltpu.CompilerParams(vmem_limit_bytes=1 << 20), name="store")(*arrays)

def solution(mesh):
    n = mesh.shape["dp"]

    def step(x, dy, wg, wu, wd, mg, mu, md, vg, vu, vd):
        s, at, dh = tokens(x, dy, wg, wu, wd)
        g, ss = grads(n, s, at, dh)
        me = lax.axis_index("dp").astype(jnp.int32).reshape(1)
        new, m, v = adam(n, me, ss, g, (wg, wu, wd), (mg, mu, md), (vg, vu, vd))
        return (*store(gather(n, new)), *m, *v)

    data, whole, rows = P(("rep", "dp"), None, None), P(None, None, None), P(None, "dp", None)
    return jax.shard_map(step, mesh=mesh, in_specs=(data,) * 2 + (whole,) * 3 + (rows,) * 6,
                         out_specs=(P("rep", None, None),) * 3 + (P("rep", "dp", None),) * 6, check_vma=False)
```

```python
import functools

import jax
import jax.numpy as jnp
from jax import lax
from jax.experimental import pallas as pl
from jax.experimental.pallas import tpu as pltpu
from jax.sharding import PartitionSpec as P

F32, BF16 = jnp.float32, jnp.bfloat16
NT = (((1,), (1,)), ((), ()))

def dot(a, b):
    return jnp.dot(a, b, preferred_element_type=F32)
def dot_t(a, b):
    return lax.dot_general(a, b, NT, preferred_element_type=F32)

def norm_of(h):
    wide = h.astype(F32)
    scale = lax.rsqrt(jnp.mean(wide * wide, -1, keepdims=True) + 1e-6)
    return wide, scale

def tokens_kernel(nf, x_ref, dy_ref, wg_hbm, wu_hbm, wd_hbm, s_ref, a_ref, dh_ref, wg, wu, wd, g0, u0, sems):
    i = pl.program_id(0)
    ff = wg.shape[2]
    fb = ff // nf
    cols = [slice(k * fb, (k + 1) * fb) for k in range(nf)]
    hbm, vm = (wg_hbm, wu_hbm, wd_hbm), (wg, wu, wd)
    def copies(l):
        return [pltpu.make_async_copy(h.at[l], v.at[l], sems.at[l, j]) for j, (h, v) in enumerate(zip(hbm, vm))]
    @pl.when(i == 0)
    def _():
        for l in range(2):
            for c in copies(l): c.start()
    def arrive(l, j):
        @pl.when(i == 0)
        def _(): copies(l)[j].wait()

    x = x_ref[0]
    wide, scale = norm_of(x)
    a0 = (wide * scale).astype(BF16)
    a_ref[1] = a0.T
    arrive(0, 0); arrive(0, 1); arrive(0, 2)
    down = None
    for c in cols:
        g = dot(a0, wg[0, :, c]); u = dot(a0, wu[0, :, c])
        g0[:, c] = g; u0[:, c] = u
        p = (g * jax.nn.sigmoid(g) * u).astype(BF16)
        s_ref[5, :, c] = p
        d = dot(p, wd[0, c, :])
        down = d if down is None else down + d
    h1 = x + down.astype(BF16)
    wide1, scale1 = norm_of(h1)
    a1 = (wide1 * scale1).astype(BF16)
    a_ref[0] = a1.T
    dy = dy_ref[0]
    dh_ref[0] = dy
    arrive(1, 0); arrive(1, 1); arrive(1, 2)
    dag = dau = None
    for c in cols:
        g = dot(a1, wg[1, :, c]); u = dot(a1, wu[1, :, c])
        dp = dot_t(dy, wd[1, c, :]).astype(BF16).astype(F32)
        sig = jax.nn.sigmoid(g); si = g * sig
        s_ref[2, :, c] = (si * u).astype(BF16)
        dg = (dp * u * (sig + si * (1 - sig))).astype(BF16)
        du = (dp * si).astype(BF16)
        s_ref[0, :, c] = dg
        s_ref[1, :, c] = du
        e = dot_t(dg, wg[1, :, c]); f = dot_t(du, wu[1, :, c])
        dag = e if dag is None else dag + e
        dau = f if dau is None else dau + f
    da = (dag.astype(BF16) + dau.astype(BF16)).astype(F32)
    coef = jnp.sum(da * wide1, -1, keepdims=True) * (scale1 * scale1 * scale1) * (-1.0 / da.shape[-1])
    dh1 = dy + (da * scale1 + wide1 * coef).astype(BF16)
    dh_ref[1] = dh1
    for c in cols:
        dp = dot_t(dh1, wd[0, c, :]).astype(BF16).astype(F32)
        g = g0[:, c]; u = u0[:, c]
        sig = jax.nn.sigmoid(g); si = g * sig
        s_ref[3, :, c] = (dp * u * (sig + si * (1 - sig))).astype(BF16)
        s_ref[4, :, c] = (dp * si).astype(BF16)

def tokens(x, dy, wg, wu, wd, tm=256, nf=3):
    _, t, d = x.shape
    ff = wg.shape[2]
    tile = pl.BlockSpec((1, tm, d), lambda i: (0, i, 0))
    anyspec = pl.BlockSpec(memory_space=pl.ANY)
    return pl.pallas_call(
        functools.partial(tokens_kernel, nf), grid=(t // tm,),
        in_specs=[tile, tile, anyspec, anyspec, anyspec],
        out_specs=[pl.BlockSpec((6, tm, ff), lambda i: (0, i, 0)), pl.BlockSpec((2, d, tm), lambda i: (0, 0, i)), pl.BlockSpec((2, tm, d), lambda i: (0, i, 0))],
        out_shape=[jax.ShapeDtypeStruct((6, t, ff), BF16), jax.ShapeDtypeStruct((2, d, t), BF16), jax.ShapeDtypeStruct((2, t, d), BF16)],
        scratch_shapes=[pltpu.VMEM(wg.shape, BF16), pltpu.VMEM(wu.shape, BF16), pltpu.VMEM(wd.shape, BF16),
                        pltpu.VMEM((tm, ff), F32), pltpu.VMEM((tm, ff), F32), pltpu.SemaphoreType.DMA((2, 3))],
        compiler_params=pltpu.CompilerParams(vmem_limit_bytes=67043328, dimension_semantics=("arbitrary",)),
        name="tokens",
    )(x, dy, wg, wu, wd)
TN = (((0,), (0,)), ((), ()))
NK = 3
RING = 11
L1, L2, L3 = 1, 3, 5

def grads_kernel(n, s_hbm, at_hbm, dh_hbm, g_ref, ss_ref, at, dh, inb, st, re, sb, rt, cb, rf, ss, ssr,
                 in_sem, ld_sem, e_s, e_r, r1_s, r1_r, r2_s, r2_r, x_s, x_r):
    me = lax.axis_index("dp")
    core, chip = lax.rem(me, 2), lax.div(me, 2)
    chips = n // 2
    mats, t, ff = s_hbm.shape
    d = at_hbm.shape[1]
    chunks = mats * NK
    cw, rg, rk = ff // NK, d // n, ff // n // NK
    rows = g_ref.shape[1]
    half = rows // 2
    A, B = pl.ds(0, half), pl.ds(half, half)
    nxt, prv, far = lax.rem(chip + 1, chips), lax.rem(chip + chips - 1, chips), lax.rem(chip + 2, chips)
    right, left, partner = nxt * 2 + core, prv * 2 + core, chip * 2 + (1 - core)

    def remote(src, dst, send, recv, to):
        return pltpu.make_async_remote_copy(src_ref=src, dst_ref=dst, send_sem=send, recv_sem=recv,
                                            device_id={"dp": to}, device_id_type=pl.DeviceIdType.MESH)

    def fetch(c):
        return pltpu.make_async_copy(s_hbm.at[lax.div(c, NK), :, pl.ds(pl.multiple_of(lax.rem(c, NK) * cw, cw), cw)],
                                     inb.at[lax.rem(c, 2)], in_sem.at[lax.rem(c, 2)])

    def loads(l):
        return (pltpu.make_async_copy(at_hbm.at[l], at, ld_sem.at[0]), pltpu.make_async_copy(dh_hbm.at[l], dh, ld_sem.at[1]))

    fetch(0).start()
    barrier = pltpu.get_barrier_semaphore()
    for o in range(1, n):
        pl.semaphore_signal(barrier, inc=1, device_id={"dp": lax.rem(me + o, n)}, device_id_type=pl.DeviceIdType.MESH)
    pl.semaphore_wait(barrier, n - 1)
    ss[...] = jnp.zeros_like(ss)

    def compute(c, _):
        mat, k = lax.div(c, NK), lax.rem(c, NK)
        layer, kind = lax.div(mat, 3), lax.rem(mat, 3)
        fresh = lax.rem(c, 3 * NK) == 0

        @pl.when(fresh)
        def _():
            for one in loads(layer):
                one.start()
        fetch(c).wait()

        @pl.when(c + 1 < chunks)
        def _():
            fetch(c + 1).start()

        @pl.when(fresh)
        def _():
            loads(layer)[0].wait()

        @pl.when(lax.rem(c, 3 * NK) == 2 * NK)
        def _():
            loads(layer)[1].wait()
        slot = lax.rem(c, 2)

        @pl.when(kind < 2)
        def _():
            out = jnp.dot(at[...], inb[slot], preferred_element_type=F32).astype(BF16)
            for b in range(n):
                for i in range(cw // 128):
                    st[lax.rem(core + b, 2), lax.rem(c, RING), b // 2, i * rg:(i + 1) * rg, :] = out[b * rg:(b + 1) * rg, i * 128:(i + 1) * 128]

        @pl.when(kind == 2)
        def _():
            def sub(j, _):
                wide = cw // 2
                out = lax.dot_general(inb[slot, :, pl.ds(pl.multiple_of(j * wide, 128), wide)], dh[...], TN, preferred_element_type=F32).astype(BF16)
                for i in range(wide // rk):
                    q = (2 * k + j) * (wide // rk) + i
                    b, part = lax.div(q, NK), lax.rem(q, NK)
                    for tile in range(d // 128):
                        st[lax.rem(core + b, 2), lax.rem(mat * NK + part, RING), lax.div(b, 2), tile * rk:(tile + 1) * rk, :] = \
                            out[i * rk:(i + 1) * rk, tile * 128:(tile + 1) * 128]
                return 0
            lax.fori_loop(0, 2, sub, 0)
        return 0

    def exchange(c):
        return remote(st.at[1, lax.rem(c, RING)], re.at[c], e_s.at[lax.rem(c, 4)], e_r.at[c], partner)

    def first(c):
        r, q = lax.rem(c, 3), lax.rem(c, 4)
        return (remote(sb.at[r, 0], rt.at[c, 0], r1_s.at[q, 0], r1_r.at[c, 0], left),
                remote(sb.at[r, 1], rt.at[c, 1], r1_s.at[q, 1], r1_r.at[c, 1], right),
                remote(sb.at[r, 2], rf.at[c, 0, B], r1_s.at[q, 2], r1_r.at[c, 2], left),
                remote(sb.at[r, 3], rf.at[c, 1, A], r1_s.at[q, 3], r1_r.at[c, 3], right))

    def second(c):
        r, q = lax.rem(c, 3), lax.rem(c, 4)
        return (remote(cb.at[r, 0], rf.at[c, 0, A], r2_s.at[q, 0], r2_r.at[c, 0], left),
                remote(cb.at[r, 1], rf.at[c, 1, B], r2_s.at[q, 1], r2_r.at[c, 1], right))

    def pair(c, to, part):
        return st[0, lax.rem(c, RING), to, part, :].astype(F32) + re[c, to, part, :].astype(F32)

    def step(s, _):
        def done(u):
            ahead = jnp.where(u >= 5, 1, 0) + jnp.where(u >= 6, 1, 0)
            return jnp.minimum(u + 1 + ahead, chunks)
        lax.fori_loop(jnp.where(s == 0, 0, done(s - 1)), done(s), compute, 0)

        @pl.when((s >= L1) & (s < chunks + L1))
        def _():
            c = s - L1
            exchange(c).wait()
            r = lax.rem(c, 3)
            sb[r, 0] = pair(c, far, A).astype(BF16)
            sb[r, 1] = pair(c, far, B).astype(BF16)
            sb[r, 2] = pair(c, prv, B).astype(BF16)
            sb[r, 3] = pair(c, nxt, A).astype(BF16)

        @pl.when((s >= L2) & (s < chunks + L2))
        def _():
            c = s - L2
            for i, one in enumerate(first(c)):
                one.wait_send()
                if i < 2:
                    one.wait_recv()
            r = lax.rem(c, 3)
            cb[r, 0] = (pair(c, prv, A) + rt[c, 0].astype(F32)).astype(BF16)
            cb[r, 1] = (pair(c, nxt, B) + rt[c, 1].astype(F32)).astype(BF16)

        @pl.when(s < chunks)
        def _():
            exchange(s).start()

        @pl.when((s >= L2) & (s < chunks + L2))
        def _():
            for one in second(s - L2):
                one.start()

        @pl.when((s >= L1) & (s < chunks + L1))
        def _():
            for one in first(s - L1):
                one.start()

        @pl.when(s >= L3)
        def _():
            c = s - L3
            for one in first(c)[2:]:
                one.wait_recv()
            for one in second(c):
                one.wait()
            g = (pair(c, chip, pl.ds(0, rows)) + rf[c, 0].astype(F32) + rf[c, 1].astype(F32)).astype(BF16)
            g_ref[c] = g
            wide = g.astype(F32)
            ss[...] += jnp.sum((wide * wide).reshape(rows // 8, 8, 128), 0)
        return 0

    lax.fori_loop(0, chunks + L3, step, 0)
    tell = [remote(ss, ssr.at[o], x_s.at[o], x_r.at[o], lax.rem(me + o, n)) for o in range(1, n)]
    for one in tell:
        one.start()
    total = ss[...]
    for o, one in enumerate(tell, 1):
        one.wait()
        total = total + ssr[o]
    ss_ref[...] = total

def grads(n, s, at, dh):
    mats, t, ff = s.shape
    d = at.shape[1]
    chunks, rows = mats * NK, ff // NK // 128 * (d // n)
    assert rows == d // 128 * (ff // n // NK)
    half, dma = rows // 2, pltpu.SemaphoreType.DMA
    anyspec = pl.BlockSpec(memory_space=pl.ANY)
    return pl.pallas_call(
        functools.partial(grads_kernel, n),
        in_specs=[anyspec] * 3,
        out_specs=[pl.BlockSpec(memory_space=pltpu.VMEM)] * 2,
        out_shape=[pltpu.VMEM((chunks, rows, 128), BF16), pltpu.VMEM((8, 128), F32)],
        scratch_shapes=[pltpu.VMEM((d, t), BF16), pltpu.VMEM((t, d), BF16), pltpu.VMEM((2, t, ff // NK), BF16),
                        pltpu.VMEM((2, RING, n // 2, rows, 128), BF16), pltpu.VMEM((chunks, n // 2, rows, 128), BF16),
                        pltpu.VMEM((3, 4, half, 128), BF16), pltpu.VMEM((chunks, 2, half, 128), BF16),
                        pltpu.VMEM((3, 2, half, 128), BF16), pltpu.VMEM((chunks, 2, rows, 128), BF16),
                        pltpu.VMEM((8, 128), F32), pltpu.VMEM((n, 8, 128), F32),
                        dma((2,)), dma((2,)), dma((4,)), dma((chunks,)), dma((4, 4)), dma((chunks, 4)), dma((4, 2)), dma((chunks, 2)),
                        dma((n,)), dma((n,))],
        compiler_params=pltpu.CompilerParams(vmem_limit_bytes=58 << 20, collective_id=0, has_side_effects=True),
        name="grads",
    )(s, at, dh)


def update_kernel(n, count, ss_ref, g_ref, *refs):
    given, outs, (in_sem, s_sem, r_sem) = refs[:9], refs[9:18], refs[18:]
    me = lax.axis_index("dp")
    chips = n // 2
    core, chip = lax.rem(me, 2), lax.div(me, 2)
    owner = lambda c, q=None: lax.rem(c + chips, chips) * 2 + (core if q is None else q)
    right, left, partner = owner(chip + 1), owner(chip - 1), owner(chip, 1 - core)
    pieces = [(i, l) for i in range(3) for l in range(2)]

    def rows_of(i, b, k=0, part=1):
        rows = outs[3 + i].shape[1]
        return pl.ds(pl.multiple_of(b * rows + k * (rows // part), 16), rows // part)

    def place(i, l, b):
        return outs[i].at[l, rows_of(i, b), :]

    def arrive(p):
        i, l = pieces[p]
        return (pltpu.make_async_copy(given[i].at[l, rows_of(i, me), :], place(i, l, me), in_sem.at[0, p]),
                pltpu.make_async_copy(given[3 + i].at[l], outs[3 + i].at[l], in_sem.at[1, p]),
                pltpu.make_async_copy(given[6 + i].at[l], outs[6 + i].at[l], in_sem.at[2, p]))
    for p in range(len(pieces)):
        for one in arrive(p):
            one.start()
    barrier = pltpu.get_barrier_semaphore()
    for to in (left, right, partner):
        pl.semaphore_signal(barrier, inc=1, device_id={"dp": to}, device_id_type=pl.DeviceIdType.MESH)
    total = jnp.sum(ss_ref[...], keepdims=True)
    factor = jnp.minimum(1.0, 0.5 * lax.rsqrt(total / count + 1e-30))

    def renew(p):
        i, l = pieces[p]
        for one in arrive(p):
            one.wait()
        full, cols = outs[3 + i].shape[1:]
        rows, tiles = (full, cols // NK // 128) if i < 2 else (full // NK, cols // 128)

        def part(k, _):
            for t in range(tiles):
                if i < 2:
                    r, own = pl.ds(0, full), rows_of(i, me)
                    c = pl.ds(pl.multiple_of(k * (cols // NK) + t * 128, 128), 128)
                else:
                    r, own = pl.ds(pl.multiple_of(k * rows, 16), rows), rows_of(i, me, k, NK)
                    c = pl.ds(t * 128, 128)
                g = g_ref[(1 - l) * 3 * NK + i * NK + k, t * rows:(t + 1) * rows, :].astype(F32) * factor
                m = 0.9 * outs[3 + i][l, r, c] + 0.1 * g
                v = 0.95 * outs[6 + i][l, r, c] + 0.05 * g * g
                w = outs[i][l, own, c].astype(F32)
                outs[i][l, own, c] = (w - 0.02 * (m * lax.rsqrt(v + 1e-8) + 0.1 * w)).astype(BF16)
                outs[3 + i][l, r, c] = m
                outs[6 + i][l, r, c] = v
            return 0
        lax.fori_loop(0, NK, part, 0)

    def copy(kind, p):
        i, l = pieces[p]
        if kind == 0:
            to, b = right, me
        elif kind == 1:
            to, b = left, me
        elif kind == 2:
            to, b = (right, owner(chip - 1)) if l == 0 else (left, owner(chip + 1))
        else:
            to = partner
            b = (me, owner(chip - 1), owner(chip + 1), owner(chip + 2))[kind - 3]
        ref = place(i, l, b)
        return pltpu.make_async_remote_copy(src_ref=ref, dst_ref=ref, send_sem=s_sem.at[kind, p], recv_sem=r_sem.at[kind, p],
                                            device_id={"dp": to}, device_id_type=pl.DeviceIdType.MESH)
    zero, one_ = [p for p, (i, l) in enumerate(pieces) if l == 0], [p for p, (i, l) in enumerate(pieces) if l == 1]
    for p in range(len(pieces)):
        renew(p)
        if p == 0:
            pl.semaphore_wait(barrier, 3)
        if p > 0:
            copy(0 if pieces[p - 1][1] == 0 else 1, p - 1).start()
    copy(1, len(pieces) - 1).start()
    for a, b in zip(zero, one_):
        copy(0, b).start()
        copy(1, a).start()
    for p in range(len(pieces)):
        copy(3, p).start()
    for a, b in zip(zero, one_):
        copy(0, a).wait_recv()
        copy(2, a).start()
        copy(4, a).start()
        copy(1, b).wait_recv()
        copy(2, b).start()
        copy(5, b).start()
    for a, b in zip(one_, zero):
        copy(0, a).wait_recv()
        copy(4, a).start()
        copy(1, b).wait_recv()
        copy(5, b).start()
    for a, b in zip(zero, one_):
        for p in (a, b):
            copy(2, p).wait_recv()
            copy(6, p).start()
    for p in range(len(pieces)):
        for kind in range(7):
            copy(kind, p).wait_send()
            if kind >= 3:
                copy(kind, p).wait_recv()

def update(n, ss, g, ws, ms, vs):
    dma, vmem = pltpu.SemaphoreType.DMA, pl.BlockSpec(memory_space=pltpu.VMEM)
    count = n * sum(m.size for m in ms)
    out = pl.pallas_call(
        functools.partial(update_kernel, n, count),
        in_specs=[vmem] * 2 + [pl.BlockSpec(memory_space=pltpu.HBM)] * 9,
        out_specs=[vmem] * 9,
        out_shape=[pltpu.VMEM(a.shape, a.dtype) for a in (*ws, *ms, *vs)],
        scratch_shapes=[dma((3, 6)), dma((7, 6)), dma((7, 6))],
        compiler_params=pltpu.CompilerParams(vmem_limit_bytes=8 << 20, collective_id=1, has_side_effects=True),
        name="update",
    )(ss, g, *(pltpu.with_memory_space_constraint(a, pltpu.HBM) for a in (*ws, *ms, *vs)))
    return out

def store_kernel(*refs):
    half = (len(refs) - 1) // 2
    copies = [pltpu.make_async_copy(refs[i], refs[half + i], refs[-1].at[i]) for i in range(half)]
    for one in copies:
        one.start()
    for one in copies:
        one.wait()

def store(arrays):
    k = len(arrays)
    return pl.pallas_call(
        store_kernel, in_specs=[pl.BlockSpec(memory_space=pltpu.VMEM)] * k, out_specs=[pl.BlockSpec(memory_space=pltpu.HBM)] * k,
        out_shape=[pltpu.HBM(a.shape, a.dtype) for a in arrays], scratch_shapes=[pltpu.SemaphoreType.DMA((k,))],
        compiler_params=pltpu.CompilerParams(vmem_limit_bytes=1 << 20), name="store")(*arrays)

def solution(mesh):
    n = mesh.shape["dp"]

    def step(x, dy, wg, wu, wd, mg, mu, md, vg, vu, vd):
        s, at, dh = tokens(x, dy, wg, wu, wd)
        g, ss = grads(n, s, at, dh)
        return tuple(store(update(n, ss, g, (wg, wu, wd), (mg, mu, md), (vg, vu, vd))))

    data, whole, rows = P(("rep", "dp"), None, None), P(None, None, None), P(None, "dp", None)
    return jax.shard_map(step, mesh=mesh, in_specs=(data,) * 2 + (whole,) * 3 + (rows,) * 6,
                         out_specs=(P("rep", None, None),) * 3 + (P("rep", "dp", None),) * 6, check_vma=False)
```

```python
import functools

import jax
import jax.numpy as jnp
from jax import lax
from jax.experimental import pallas as pl
from jax.experimental.pallas import tpu as pltpu
from jax.sharding import PartitionSpec as P

F32, BF16 = jnp.float32, jnp.bfloat16
NT = (((1,), (1,)), ((), ()))

def dot(a, b):
    return jnp.dot(a, b, preferred_element_type=F32)
def dot_t(a, b):
    return lax.dot_general(a, b, NT, preferred_element_type=F32)

def norm_of(h):
    wide = h.astype(F32)
    scale = lax.rsqrt(jnp.mean(wide * wide, -1, keepdims=True) + 1e-6)
    return wide, scale

def sigmoid(g):
    return 0.5 * jnp.tanh(0.5 * g) + 0.5

def swiglu_back(dp, g, u):
    sig = sigmoid(g)
    si = g * sig
    return (dp * u * (sig + si - si * sig)).astype(BF16), (dp * si).astype(BF16), (si * u).astype(BF16)

def tokens_kernel(nf, x_ref, dy_ref, wg_hbm, wu_hbm, wd_hbm, s_ref, gu_ref, at_ref, h_ref, wg, wu, wd, sems):
    i = pl.program_id(0)
    ff = wg.shape[2]
    fb = ff // nf
    cols = [slice(k * fb, (k + 1) * fb) for k in range(nf)]
    copies = {(l, j): pltpu.make_async_copy(h.at[l], v.at[l], sems.at[l, j])
              for l in range(2) for j, (h, v) in enumerate(((wg_hbm, wg), (wu_hbm, wu), (wd_hbm, wd)))}

    @pl.when(i == 0)
    def _():
        for one in copies.values():
            one.start()

    def arrive(*which):
        @pl.when(i == 0)
        def _():
            for one in which:
                copies[one].wait()

    x = x_ref[0]
    wide, scale = norm_of(x)
    a0 = (wide * scale).astype(BF16)
    at_ref[1] = a0.T
    arrive((0, 0), (0, 1), (0, 2))
    down = None
    for c in cols:
        g, u = dot(a0, wg[0, :, c]), dot(a0, wu[0, :, c])
        gu_ref[0, :, c] = g
        gu_ref[1, :, c] = u
        p = (g * sigmoid(g) * u).astype(BF16)
        s_ref[3, :, c] = p
        d = dot(p, wd[0, c, :])
        down = d if down is None else down + d
    h1 = x + down.astype(BF16)
    h_ref[...] = h1
    wide, scale = norm_of(h1)
    a1 = (wide * scale).astype(BF16)
    at_ref[0] = a1.T
    dy = dy_ref[0]
    arrive((1, 0), (1, 1), (1, 2))
    for c in cols:
        g, u = dot(a1, wg[1, :, c]), dot(a1, wu[1, :, c])
        dp = dot_t(dy, wd[1, c, :]).astype(BF16).astype(F32)
        s_ref[0, :, c], s_ref[1, :, c], s_ref[2, :, c] = swiglu_back(dp, g, u)

def tokens(x, dy, wg, wu, wd, tm=256, nf=3):
    _, t, d = x.shape
    ff = wg.shape[2]
    tile = pl.BlockSpec((1, tm, d), lambda i: (0, i, 0))
    anyspec = pl.BlockSpec(memory_space=pl.ANY)
    wide = lambda k: pl.BlockSpec((k, tm, ff), lambda i: (0, i, 0))
    return pl.pallas_call(
        functools.partial(tokens_kernel, nf), grid=(t // tm,),
        in_specs=[tile, tile, anyspec, anyspec, anyspec],
        out_specs=[wide(4), wide(2), pl.BlockSpec((2, d, tm), lambda i: (0, 0, i)), pl.BlockSpec((tm, d), lambda i: (i, 0))],
        out_shape=[jax.ShapeDtypeStruct((4, t, ff), BF16), jax.ShapeDtypeStruct((2, t, ff), F32),
                   jax.ShapeDtypeStruct((2, d, t), BF16), jax.ShapeDtypeStruct((t, d), BF16)],
        scratch_shapes=[pltpu.VMEM(wg.shape, BF16), pltpu.VMEM(wu.shape, BF16), pltpu.VMEM(wd.shape, BF16), pltpu.SemaphoreType.DMA((2, 3))],
        compiler_params=pltpu.CompilerParams(vmem_limit_bytes=67043328, dimension_semantics=("arbitrary",)),
        name="tokens",
    )(x, dy, wg, wu, wd)

TN = (((0,), (0,)), ((), ()))
NK, RING, AHEAD = 3, 9, 5
L1, L2, L3 = 1, 3, 5
WHEN = (*range(6), 5, 6, *range(6, 12), 11, *range(11, 18))
SEND = (*range(9), 11, *range(11, 13), *range(12, 18))
PENDING = 6

def grads_kernel(n, s_hbm, gu_hbm, at_hbm, h_hbm, dy_hbm, wg_hbm, wu_hbm, wd_hbm, g_ref, ss_ref,
                 at, dh, inb, w1, wdb, gub, hb, gout, st, re, sb, rt, cb, rf, ss, ssr,
                 in_sem, ld_sem, gu_sem, b_sem, g_sem, e_s, e_r, r1_s, r1_r, r2_s, r2_r, x_s, x_r, free):
    me = lax.axis_index("dp")
    core, chip = lax.rem(me, 2), lax.div(me, 2)
    chips = n // 2
    t, d = dh.shape
    ff = wg_hbm.shape[2]
    chunks, rows = g_ref.shape[:2]
    slots = chunks // 2
    cw, rg, rk = ff // NK, d // n, ff // n // NK
    half = rows // 2
    A, B = pl.ds(0, half), pl.ds(half, half)
    nxt, prv, far = lax.rem(chip + 1, chips), lax.rem(chip + chips - 1, chips), lax.rem(chip + 2, chips)
    right, left, partner = nxt * 2 + core, prv * 2 + core, chip * 2 + (1 - core)

    def remote(src, dst, send, recv, to):
        return pltpu.make_async_remote_copy(src_ref=src, dst_ref=dst, send_sem=send, recv_sem=recv,
                                            device_id={"dp": to}, device_id_type=pl.DeviceIdType.MESH)

    def fetch(c):
        return pltpu.make_async_copy(s_hbm.at[lax.div(c, NK), :, pl.ds(pl.multiple_of(lax.rem(c, NK) * cw, cw), cw)],
                                     inb.at[lax.rem(c, 2)], in_sem.at[lax.rem(c, 2)])

    def down(k):
        return pltpu.make_async_copy(wd_hbm.at[0, pl.ds(pl.multiple_of(k * cw, cw), cw), :], wdb, ld_sem.at[2])

    quarter = t // 4

    def saved(q, one):
        return pltpu.make_async_copy(
            gu_hbm.at[one, pl.ds(pl.multiple_of(lax.rem(q, 4) * quarter, quarter), quarter), pl.ds(pl.multiple_of(lax.div(q, 4) * cw, cw), cw)],
            gub.at[lax.rem(q, 2), one], gu_sem.at[one, lax.rem(q, 2)])

    def cotangent(q, one):
        return [pltpu.make_async_copy(s_hbm.at[one, pl.ds(pl.multiple_of(q * quarter, quarter), quarter), pl.ds(k * cw, cw)],
                                      inb.at[one, pl.ds(k * quarter, quarter), :], b_sem.at[one, k]) for k in range(NK)]

    def state(q):
        return pltpu.make_async_copy(h_hbm.at[pl.ds(pl.multiple_of(q * quarter, quarter), quarter), :], hb, b_sem.at[2, 0])

    w1_load = [pltpu.make_async_copy(w.at[1], w1.at[one], b_sem.at[2, 1 + one]) for one, w in enumerate((wg_hbm, wu_hbm))]
    at_load = [pltpu.make_async_copy(at_hbm.at[l], at, ld_sem.at[0]) for l in range(2)]
    dy_load = pltpu.make_async_copy(dy_hbm.at[0], dh, ld_sem.at[1])
    at_load[0].start()
    fetch(0).start()
    barrier = pltpu.get_barrier_semaphore()
    for o in range(1, n):
        pl.semaphore_signal(barrier, inc=1, device_id={"dp": lax.rem(me + o, n)}, device_id_type=pl.DeviceIdType.MESH)
    pl.semaphore_wait(barrier, n - 1)
    ss[...] = jnp.zeros_like(ss)

    def place(other, c):
        return (1 - other) * lax.rem(c, RING) + other * (RING + lax.rem(c, AHEAD))

    def back_through_norm(q):
        @pl.when(q == 0)
        def _():
            for one in (*cotangent(0, 0), *cotangent(0, 1), state(0)):
                one.start()
            for one in w1_load:
                one.wait()
        parts = []
        for one in range(2):
            for copy in cotangent(q, one):
                copy.wait()
            total = sum(dot_t(inb[one, k * quarter:(k + 1) * quarter, :], w1[one, :, k * cw:(k + 1) * cw]) for k in range(NK))
            parts.append(total.astype(BF16))

            @pl.when(q < 3)
            def _():
                for copy in cotangent(q + 1, one):
                    copy.start()
        state(q).wait()
        r = pl.ds(pl.multiple_of(q * quarter, quarter), quarter)
        wide, scale = norm_of(hb[...])
        da = (parts[0] + parts[1]).astype(F32)
        coef = jnp.sum(da * wide, -1, keepdims=True) * (scale * scale * scale) * (-1.0 / d)
        dh[r, :] = dh[r, :] + (da * scale + wide * coef).astype(BF16)

        @pl.when(q < 3)
        def _():
            state(q + 1).start()

        @pl.when(q == 3)
        def _():
            fetch(3 * NK).start()
            down(0).start()
            for one in range(2):
                saved(0, one).start()

    def back_to_hidden(k):
        down(k).wait()

        def tile(j, _):
            q = 4 * k + j
            for one in range(2):
                saved(q, one).wait()

            @pl.when(q < 4 * NK - 1)
            def _():
                for one in range(2):
                    saved(q + 1, one).start()
            r = pl.ds(pl.multiple_of(j * quarter, quarter), quarter)
            for p in range(NK):
                part = slice(p * (cw // NK), (p + 1) * (cw // NK))
                dp = dot_t(dh[r, :], wdb[part, :]).astype(BF16).astype(F32)
                inb[0, r, part], inb[1, r, part], _ = swiglu_back(dp, gub[lax.rem(q, 2), 0, :, part], gub[lax.rem(q, 2), 1, :, part])
            return 0
        lax.fori_loop(0, 4, tile, 0)

        @pl.when(k < NK - 1)
        def _():
            down(k + 1).start()

    def compute(item, _):
        first, last = item < 3 * NK, item >= 3 * NK + 4

        @pl.when(first | last)
        def _():
            chunk(jnp.where(first, item, item - 4))

        @pl.when((item >= 3 * NK) & (item < 3 * NK + 4))
        def _():
            back_through_norm(item - 3 * NK)
        return 0

    def chunk(c):
        k, slot = lax.rem(c, NK), lax.rem(c, 2)
        wide_kind = (c < 2 * NK) | (c >= 4 * NK)

        @pl.when(c == 0)
        def _():
            at_load[0].wait()
            dy_load.start()

        @pl.when(c == 1)
        def _():
            for one in w1_load:
                one.start()

        @pl.when(c == 2 * NK)
        def _():
            dy_load.wait()
            at_load[1].start()

        @pl.when(c == 4 * NK)
        def _():
            at_load[1].wait()

        @pl.when(c < 4 * NK)
        def _():
            fetch(c).wait()

        @pl.when((c + 1 < 4 * NK) & (c + 1 != 3 * NK))
        def _():
            fetch(c + 1).start()

        @pl.when((c >= 4 * NK) & (slot == 0))
        def _():
            back_to_hidden(lax.div(c - 4 * NK, 2))

        @pl.when(wide_kind)
        def _():
            out = dot(at[...], inb[slot]).astype(BF16)
            for b in range(n):
                for i in range(cw // 128):
                    st[place(lax.rem(core + b, 2), c), b // 2, i * rg:(i + 1) * rg, :] = out[b * rg:(b + 1) * rg, i * 128:(i + 1) * 128]

        @pl.when((c >= 2 * NK) & (c < 4 * NK))
        def _():
            def sub(j, _):
                wide = cw // 2
                out = lax.dot_general(inb[slot, :, pl.ds(pl.multiple_of(j * wide, 128), wide)], dh[...], TN, preferred_element_type=F32).astype(BF16)
                for i in range(wide // rk):
                    q = (2 * k + j) * (wide // rk) + i
                    b, part = lax.div(q, NK), lax.rem(q, NK)
                    for tile in range(d // 128):
                        st[place(lax.rem(core + b, 2), c - k + part), lax.div(b, 2), tile * rk:(tile + 1) * rk, :] = \
                            out[i * rk:(i + 1) * rk, tile * 128:(tile + 1) * 128]
                return 0
            lax.fori_loop(0, 2, sub, 0)

    def exchange(c):
        return remote(st.at[place(1, c)], re.at[lax.rem(c, slots)], e_s.at[lax.rem(c, PENDING)], e_r.at[c], partner)

    def first(c):
        r, q, v = lax.rem(c, PENDING), lax.rem(c, PENDING), lax.rem(c, slots)
        return (remote(sb.at[r, 0], rt.at[v, 0], r1_s.at[q, 0], r1_r.at[c, 0], left),
                remote(sb.at[r, 1], rt.at[v, 1], r1_s.at[q, 1], r1_r.at[c, 1], right),
                remote(sb.at[r, 2], rf.at[v, 0, B], r1_s.at[q, 2], r1_r.at[c, 2], left),
                remote(sb.at[r, 3], rf.at[v, 1, A], r1_s.at[q, 3], r1_r.at[c, 3], right))

    def second(c):
        r, q, v = lax.rem(c, PENDING), lax.rem(c, PENDING), lax.rem(c, slots)
        return (remote(cb.at[r, 0], rf.at[v, 0, A], r2_s.at[q, 0], r2_r.at[c, 0], left),
                remote(cb.at[r, 1], rf.at[v, 1, B], r2_s.at[q, 1], r2_r.at[c, 1], right))

    def keep(c):
        return pltpu.make_async_copy(gout.at[lax.rem(c, 2)], g_ref.at[c], g_sem.at[lax.rem(c, 2)])

    def pair(c, to, part):
        return st[place(0, c), to, part, :].astype(F32) + re[lax.rem(c, slots), to, part, :].astype(F32)

    def step(s, _):
        def done(u):
            return sum(jnp.where(u >= at_, 1, 0) for at_ in WHEN)

        def sent(u):
            return sum(jnp.where(u >= at_, 1, 0) for at_ in SEND)

        def each(lag):
            def run(stage):
                def one(c, _):
                    stage(c)
                    return 0
                lax.fori_loop(sent(s - lag - 1), sent(s - lag), one, 0)
            return run

        lax.fori_loop(jnp.where(s == 0, 0, done(s - 1)), done(s), compute, 0)

        @each(L1)
        def _(c):
            exchange(c).wait()
            r = lax.rem(c, PENDING)
            sb[r, 0] = pair(c, far, A).astype(BF16)
            sb[r, 1] = pair(c, far, B).astype(BF16)
            sb[r, 2] = pair(c, prv, B).astype(BF16)
            sb[r, 3] = pair(c, nxt, A).astype(BF16)

        @each(L2)
        def _(c):
            for i, one in enumerate(first(c)):
                one.wait_send()
                if i < 2:
                    one.wait_recv()
            r = lax.rem(c, PENDING)
            cb[r, 0] = (pair(c, prv, A) + rt[lax.rem(c, slots), 0].astype(F32)).astype(BF16)
            cb[r, 1] = (pair(c, nxt, B) + rt[lax.rem(c, slots), 1].astype(F32)).astype(BF16)

        @each(0)
        def _(c):

            @pl.when(c >= slots)
            def _():
                pl.semaphore_wait(free.at[0], 1)
            exchange(c).start()

        @each(L2)
        def _(c):
            for one in second(c):
                one.start()

        @each(L1)
        def _(c):

            @pl.when(c >= slots)
            def _():
                pl.semaphore_wait(free.at[1], 1)
                pl.semaphore_wait(free.at[2], 1)
            for one in first(c):
                one.start()

        @each(L3)
        def _(c):
            for one in first(c)[2:]:
                one.wait_recv()
            for one in second(c):
                one.wait()
            g = (pair(c, chip, pl.ds(0, rows)) + rf[lax.rem(c, slots), 0].astype(F32) + rf[lax.rem(c, slots), 1].astype(F32)).astype(BF16)
            @pl.when(c >= 2)
            def _():
                keep(c - 2).wait()
            gout[lax.rem(c, 2)] = g
            keep(c).start()
            wide = g.astype(F32)
            ss[...] += jnp.sum((wide * wide).reshape(rows // 8, 8, 128), 0)

            @pl.when(c < chunks - slots)
            def _():
                for i, to in enumerate((partner, right, left)):
                    pl.semaphore_signal(free.at[i], inc=1, device_id={"dp": to}, device_id_type=pl.DeviceIdType.MESH)
        return 0

    lax.fori_loop(0, SEND[-1] + 1 + L3, step, 0)
    for c in (chunks - 2, chunks - 1):
        keep(c).wait()
    tell = [remote(ss, ssr.at[o], x_s.at[o], x_r.at[o], lax.rem(me + o, n)) for o in range(1, n)]
    for one in tell:
        one.start()
    total = ss[...]
    for o, one in enumerate(tell, 1):
        one.wait()
        total = total + ssr[o]
    ss_ref[...] = total

def grads(n, s, gu, at, h, dy, wg, wu, wd):
    t, d = h.shape
    ff = wg.shape[2]
    chunks, rows = 6 * NK, ff // NK // 128 * (d // n)
    assert rows == d // 128 * (ff // n // NK)
    half, slots, dma = rows // 2, chunks // 2, pltpu.SemaphoreType.DMA
    hbm = lambda a: pltpu.with_memory_space_constraint(a, pltpu.HBM)
    return pl.pallas_call(
        functools.partial(grads_kernel, n),
        in_specs=[pl.BlockSpec(memory_space=pltpu.HBM)] * 8,
        out_specs=[pl.BlockSpec(memory_space=pltpu.HBM), pl.BlockSpec(memory_space=pltpu.VMEM)],
        out_shape=[pltpu.HBM((chunks, rows, 128), BF16), pltpu.VMEM((8, 128), F32)],
        scratch_shapes=[pltpu.VMEM((d, t), BF16), pltpu.VMEM((t, d), BF16), pltpu.VMEM((2, t, ff // NK), BF16),
                        pltpu.VMEM((2, d, ff), BF16), pltpu.VMEM((ff // NK, d), BF16), pltpu.VMEM((2, 2, t // 4, ff // NK), F32),
                        pltpu.VMEM((t // 4, d), BF16), pltpu.VMEM((2, rows, 128), BF16),
                        pltpu.VMEM((RING + AHEAD, n // 2, rows, 128), BF16), pltpu.VMEM((slots, n // 2, rows, 128), BF16),
                        pltpu.VMEM((PENDING, 4, half, 128), BF16), pltpu.VMEM((slots, 2, half, 128), BF16),
                        pltpu.VMEM((PENDING, 2, half, 128), BF16), pltpu.VMEM((slots, 2, rows, 128), BF16),
                        pltpu.VMEM((8, 128), F32), pltpu.VMEM((n, 8, 128), F32),
                        dma((2,)), dma((3,)), dma((2, 2)), dma((3, 3)), dma((2,)), dma((PENDING,)), dma((chunks,)), dma((PENDING, 4)), dma((chunks, 4)),
                        dma((PENDING, 2)), dma((chunks, 2)), dma((n,)), dma((n,)), pltpu.SemaphoreType.REGULAR((3,))],
        compiler_params=pltpu.CompilerParams(vmem_limit_bytes=60 << 20, collective_id=0, has_side_effects=True),
        name="grads",
    )(*(hbm(a) for a in (s, gu, at, h, dy, wg, wu, wd)))


def update_kernel(n, count, ss_ref, g_hbm, *refs):
    given, outs, (g_ref, in_sem, g_sem, s_sem, r_sem) = refs[:9], refs[9:18], refs[18:]
    me = lax.axis_index("dp")
    chips = n // 2
    core, chip = lax.rem(me, 2), lax.div(me, 2)
    owner = lambda c, q=None: lax.rem(c + chips, chips) * 2 + (core if q is None else q)
    right, left, partner = owner(chip + 1), owner(chip - 1), owner(chip, 1 - core)
    pieces = [(i, l) for i in range(3) for l in range(2)]

    def rows_of(i, b, k=0, part=1):
        rows = outs[3 + i].shape[1]
        return pl.ds(pl.multiple_of(b * rows + k * (rows // part), 16), rows // part)

    def place(i, l, b):
        return outs[i].at[l, rows_of(i, b), :]

    def chunk_of(i, l, k):
        return i * NK + k if l else 3 * NK + k if i == 2 else 4 * NK + 2 * k + i

    def arrive(p):
        i, l = pieces[p]
        return (pltpu.make_async_copy(given[i].at[l, rows_of(i, me), :], place(i, l, me), in_sem.at[0, p]),
                pltpu.make_async_copy(given[3 + i].at[l], outs[3 + i].at[l], in_sem.at[1, p]),
                pltpu.make_async_copy(given[6 + i].at[l], outs[6 + i].at[l], in_sem.at[2, p]),
                *(pltpu.make_async_copy(g_hbm.at[chunk_of(i, l, k)], g_ref.at[chunk_of(i, l, k)], g_sem.at[p, k]) for k in range(NK)))
    for p in range(2):
        for one in arrive(p):
            one.start()
    barrier = pltpu.get_barrier_semaphore()
    for to in (left, right, partner):
        pl.semaphore_signal(barrier, inc=1, device_id={"dp": to}, device_id_type=pl.DeviceIdType.MESH)
    total = jnp.sum(ss_ref[...], keepdims=True)
    factor = jnp.minimum(1.0, 0.5 * lax.rsqrt(total / count + 1e-30))

    def renew(p):
        i, l = pieces[p]
        for one in arrive(p):
            one.wait()
        if p + 2 < len(pieces):
            for one in arrive(p + 2):
                one.start()
        full, cols = outs[3 + i].shape[1:]
        rows, tiles = (full, cols // NK // 128) if i < 2 else (full // NK, cols // 128)

        def part(k, _):
            for t in range(tiles):
                if i < 2:
                    r, own = pl.ds(0, full), rows_of(i, me)
                    c = pl.ds(pl.multiple_of(k * (cols // NK) + t * 128, 128), 128)
                else:
                    r, own = pl.ds(pl.multiple_of(k * rows, 16), rows), rows_of(i, me, k, NK)
                    c = pl.ds(t * 128, 128)
                g = g_ref[chunk_of(i, l, k), t * rows:(t + 1) * rows, :].astype(F32) * factor
                m = 0.9 * outs[3 + i][l, r, c] + 0.1 * g
                v = 0.95 * outs[6 + i][l, r, c] + 0.05 * g * g
                w = outs[i][l, own, c].astype(F32)
                outs[i][l, own, c] = (w - 0.02 * (m * lax.rsqrt(v + 1e-8) + 0.1 * w)).astype(BF16)
                outs[3 + i][l, r, c] = m
                outs[6 + i][l, r, c] = v
            return 0
        lax.fori_loop(0, NK, part, 0)

    def copy(kind, p):
        i, l = pieces[p]
        if kind == 0:
            to, b = right, me
        elif kind == 1:
            to, b = left, me
        elif kind == 2:
            to, b = (right, owner(chip - 1)) if l == 0 else (left, owner(chip + 1))
        else:
            to = partner
            b = (me, owner(chip - 1), owner(chip + 1), owner(chip + 2))[kind - 3]
        ref = place(i, l, b)
        return pltpu.make_async_remote_copy(src_ref=ref, dst_ref=ref, send_sem=s_sem.at[kind, p], recv_sem=r_sem.at[kind, p],
                                            device_id={"dp": to}, device_id_type=pl.DeviceIdType.MESH)
    zero, one_ = [p for p, (i, l) in enumerate(pieces) if l == 0], [p for p, (i, l) in enumerate(pieces) if l == 1]
    for p in range(len(pieces)):
        renew(p)
        if p == 0:
            pl.semaphore_wait(barrier, 3)
        if p > 0:
            copy(0 if pieces[p - 1][1] == 0 else 1, p - 1).start()
    copy(1, len(pieces) - 1).start()
    for a, b in zip(zero, one_):
        copy(0, b).start()
        copy(1, a).start()
    for p in range(len(pieces)):
        copy(3, p).start()
    for a, b in zip(zero, one_):
        copy(0, a).wait_recv()
        copy(2, a).start()
        copy(4, a).start()
        copy(1, b).wait_recv()
        copy(2, b).start()
        copy(5, b).start()
    for a, b in zip(one_, zero):
        copy(0, a).wait_recv()
        copy(4, a).start()
        copy(1, b).wait_recv()
        copy(5, b).start()
    for a, b in zip(zero, one_):
        for p in (a, b):
            copy(2, p).wait_recv()
            copy(6, p).start()
    for p in range(len(pieces)):
        for kind in range(7):
            copy(kind, p).wait_send()
            if kind >= 3:
                copy(kind, p).wait_recv()

def update(n, ss, g, ws, ms, vs):
    dma, vmem = pltpu.SemaphoreType.DMA, pl.BlockSpec(memory_space=pltpu.VMEM)
    count = n * sum(m.size for m in ms)
    out = pl.pallas_call(
        functools.partial(update_kernel, n, count),
        in_specs=[vmem] + [pl.BlockSpec(memory_space=pltpu.HBM)] * 10,
        out_specs=[vmem] * 9,
        out_shape=[pltpu.VMEM(a.shape, a.dtype) for a in (*ws, *ms, *vs)],
        scratch_shapes=[pltpu.VMEM(g.shape, BF16), dma((3, 6)), dma((6, NK)), dma((7, 6)), dma((7, 6))],
        compiler_params=pltpu.CompilerParams(vmem_limit_bytes=8 << 20, collective_id=1, has_side_effects=True),
        name="update",
    )(ss, *(pltpu.with_memory_space_constraint(a, pltpu.HBM) for a in (g, *ws, *ms, *vs)))
    return out

def store_kernel(*refs):
    half = (len(refs) - 1) // 2
    copies = [pltpu.make_async_copy(refs[i], refs[half + i], refs[-1].at[i]) for i in range(half)]
    for one in copies:
        one.start()
    for one in copies:
        one.wait()

def store(arrays):
    k = len(arrays)
    return pl.pallas_call(
        store_kernel, in_specs=[pl.BlockSpec(memory_space=pltpu.VMEM)] * k, out_specs=[pl.BlockSpec(memory_space=pltpu.HBM)] * k,
        out_shape=[pltpu.HBM(a.shape, a.dtype) for a in arrays], scratch_shapes=[pltpu.SemaphoreType.DMA((k,))],
        compiler_params=pltpu.CompilerParams(vmem_limit_bytes=1 << 20), name="store")(*arrays)

def solution(mesh):
    n = mesh.shape["dp"]

    def step(x, dy, wg, wu, wd, mg, mu, md, vg, vu, vd):
        s, gu, at, h = tokens(x, dy, wg, wu, wd)
        g, ss = grads(n, s, gu, at, h, dy, wg, wu, wd)
        return tuple(store(update(n, ss, g, (wg, wu, wd), (mg, mu, md), (vg, vu, vd))))

    data, whole, rows = P(("rep", "dp"), None, None), P(None, None, None), P(None, "dp", None)
    return jax.shard_map(step, mesh=mesh, in_specs=(data,) * 2 + (whole,) * 3 + (rows,) * 6,
                         out_specs=(P("rep", None, None),) * 3 + (P("rep", "dp", None),) * 6, check_vma=False)
```

```python
import functools

import jax
import jax.numpy as jnp
from jax import lax
from jax.experimental import pallas as pl
from jax.experimental.pallas import tpu as pltpu
from jax.sharding import PartitionSpec as P

F32, BF16 = jnp.float32, jnp.bfloat16
NT = (((1,), (1,)), ((), ()))

def dot(a, b):
    return jnp.dot(a, b, preferred_element_type=F32)
def dot_t(a, b):
    return lax.dot_general(a, b, NT, preferred_element_type=F32)

def norm_of(h):
    wide = h.astype(F32)
    scale = lax.rsqrt(jnp.mean(wide * wide, -1, keepdims=True) + 1e-6)
    return wide, scale

def sigmoid(g):
    return 0.5 * jnp.tanh(0.5 * g) + 0.5

def swiglu_back(dp, g, u):
    sig = sigmoid(g)
    si = g * sig
    return (dp * u * (sig + si - si * sig)).astype(BF16), (dp * si).astype(BF16), (si * u).astype(BF16)

def tokens_kernel(nf, x_ref, dy_ref, wg_hbm, wu_hbm, wd_hbm, s_ref, gu_ref, at_ref, h_ref, wg, wu, wd, sems):
    i = pl.program_id(0)
    ff = wg.shape[2]
    fb = ff // nf
    cols = [slice(k * fb, (k + 1) * fb) for k in range(nf)]
    copies = {(l, j): pltpu.make_async_copy(h.at[l], v.at[l], sems.at[l, j])
              for l in range(2) for j, (h, v) in enumerate(((wg_hbm, wg), (wu_hbm, wu), (wd_hbm, wd)))}

    @pl.when(i == 0)
    def _():
        for one in copies.values():
            one.start()

    def arrive(*which):
        @pl.when(i == 0)
        def _():
            for one in which:
                copies[one].wait()

    x = x_ref[0]
    wide, scale = norm_of(x)
    a0 = (wide * scale).astype(BF16)
    at_ref[1] = a0.T
    arrive((0, 0), (0, 1), (0, 2))
    down = None
    for c in cols:
        g, u = dot(a0, wg[0, :, c]), dot(a0, wu[0, :, c])
        gu_ref[0, :, c] = g
        gu_ref[1, :, c] = u
        p = (g * sigmoid(g) * u).astype(BF16)
        s_ref[3, :, c] = p
        d = dot(p, wd[0, c, :])
        down = d if down is None else down + d
    h1 = x + down.astype(BF16)
    h_ref[...] = h1
    wide, scale = norm_of(h1)
    a1 = (wide * scale).astype(BF16)
    at_ref[0] = a1.T
    dy = dy_ref[0]
    arrive((1, 0), (1, 1), (1, 2))
    for c in cols:
        g, u = dot(a1, wg[1, :, c]), dot(a1, wu[1, :, c])
        dp = dot_t(dy, wd[1, c, :]).astype(BF16).astype(F32)
        s_ref[0, :, c], s_ref[1, :, c], s_ref[2, :, c] = swiglu_back(dp, g, u)

def tokens(x, dy, wg, wu, wd, tm=256, nf=3):
    _, t, d = x.shape
    ff = wg.shape[2]
    tile = pl.BlockSpec((1, tm, d), lambda i: (0, i, 0))
    anyspec = pl.BlockSpec(memory_space=pl.ANY)
    wide = lambda k: pl.BlockSpec((k, tm, ff), lambda i: (0, i, 0))
    return pl.pallas_call(
        functools.partial(tokens_kernel, nf), grid=(t // tm,),
        in_specs=[tile, tile, anyspec, anyspec, anyspec],
        out_specs=[wide(4), wide(2), pl.BlockSpec((2, d, tm), lambda i: (0, 0, i)), pl.BlockSpec((tm, d), lambda i: (i, 0))],
        out_shape=[jax.ShapeDtypeStruct((4, t, ff), BF16), jax.ShapeDtypeStruct((2, t, ff), F32),
                   jax.ShapeDtypeStruct((2, d, t), BF16), jax.ShapeDtypeStruct((t, d), BF16)],
        scratch_shapes=[pltpu.VMEM(wg.shape, BF16), pltpu.VMEM(wu.shape, BF16), pltpu.VMEM(wd.shape, BF16), pltpu.SemaphoreType.DMA((2, 3))],
        compiler_params=pltpu.CompilerParams(vmem_limit_bytes=67043328, dimension_semantics=("arbitrary",)),
        name="tokens",
    )(x, dy, wg, wu, wd)

TN = (((0,), (0,)), ((), ()))
NK, RING, AHEAD = 3, 9, 5
L1, L2, L3 = 1, 3, 6
WHEN = (*range(6), 5, 6, *range(6, 12), 11, *range(11, 18))
SEND = (*range(9), 11, *range(11, 13), *range(12, 18))
PENDING = 6

def grads_kernel(n, s_hbm, gu_hbm, at_hbm, h_hbm, dy_hbm, wg_hbm, wu_hbm, wd_hbm, g_ref, ss_ref,
                 at, dh, inb, w1, wdb, gub, hb, gout, st, re, sb, rt, cb, rf, ss, ssr,
                 in_sem, ld_sem, gu_sem, b_sem, g_sem, e_s, e_r, r1_s, r1_r, r2_s, r2_r, x_s, x_r, free):
    me = lax.axis_index("dp")
    core, chip = lax.rem(me, 2), lax.div(me, 2)
    chips = n // 2
    t, d = dh.shape
    ff = wg_hbm.shape[2]
    chunks, rows = g_ref.shape[:2]
    slots = chunks // 2
    cw, rg, rk = ff // NK, d // n, ff // n // NK
    half = rows // 2
    A, B = pl.ds(0, half), pl.ds(half, half)
    nxt, prv, far = lax.rem(chip + 1, chips), lax.rem(chip + chips - 1, chips), lax.rem(chip + 2, chips)
    right, left, partner = nxt * 2 + core, prv * 2 + core, chip * 2 + (1 - core)

    def remote(src, dst, send, recv, to):
        return pltpu.make_async_remote_copy(src_ref=src, dst_ref=dst, send_sem=send, recv_sem=recv,
                                            device_id={"dp": to}, device_id_type=pl.DeviceIdType.MESH)

    def fetch(c):
        return pltpu.make_async_copy(s_hbm.at[lax.div(c, NK), :, pl.ds(pl.multiple_of(lax.rem(c, NK) * cw, cw), cw)],
                                     inb.at[lax.rem(c, 2)], in_sem.at[lax.rem(c, 2)])

    def down(k):
        return pltpu.make_async_copy(wd_hbm.at[0, pl.ds(pl.multiple_of(k * cw, cw), cw), :], wdb, ld_sem.at[2])

    quarter = t // 4

    def saved(q, one):
        return pltpu.make_async_copy(
            gu_hbm.at[one, pl.ds(pl.multiple_of(lax.rem(q, 4) * quarter, quarter), quarter), pl.ds(pl.multiple_of(lax.div(q, 4) * cw, cw), cw)],
            gub.at[lax.rem(q, 2), one], gu_sem.at[one, lax.rem(q, 2)])

    def cotangent(q, one):
        return [pltpu.make_async_copy(s_hbm.at[one, pl.ds(pl.multiple_of(q * quarter, quarter), quarter), pl.ds(k * cw, cw)],
                                      inb.at[one, pl.ds(k * quarter, quarter), :], b_sem.at[one, k]) for k in range(NK)]

    def state(q):
        return pltpu.make_async_copy(h_hbm.at[pl.ds(pl.multiple_of(q * quarter, quarter), quarter), :], hb, b_sem.at[2, 0])

    w1_load = [pltpu.make_async_copy(w.at[1], w1.at[one], b_sem.at[2, 1 + one]) for one, w in enumerate((wg_hbm, wu_hbm))]
    at_load = [pltpu.make_async_copy(at_hbm.at[l], at, ld_sem.at[0]) for l in range(2)]
    dy_load = pltpu.make_async_copy(dy_hbm.at[0], dh, ld_sem.at[1])
    at_load[0].start()
    fetch(0).start()
    barrier = pltpu.get_barrier_semaphore()
    for o in range(1, n):
        pl.semaphore_signal(barrier, inc=1, device_id={"dp": lax.rem(me + o, n)}, device_id_type=pl.DeviceIdType.MESH)
    pl.semaphore_wait(barrier, n - 1)
    ss[...] = jnp.zeros_like(ss)

    def place(other, c):
        return (1 - other) * lax.rem(c, RING) + other * (RING + lax.rem(c, AHEAD))

    def back_through_norm(q):
        @pl.when(q == 0)
        def _():
            for one in (*cotangent(0, 0), *cotangent(0, 1), state(0)):
                one.start()
            for one in w1_load:
                one.wait()
        parts = []
        for one in range(2):
            for copy in cotangent(q, one):
                copy.wait()
            total = sum(dot_t(inb[one, k * quarter:(k + 1) * quarter, :], w1[one, :, k * cw:(k + 1) * cw]) for k in range(NK))
            parts.append(total.astype(BF16))

            @pl.when(q < 3)
            def _():
                for copy in cotangent(q + 1, one):
                    copy.start()
        state(q).wait()
        r = pl.ds(pl.multiple_of(q * quarter, quarter), quarter)
        wide, scale = norm_of(hb[...])
        da = (parts[0] + parts[1]).astype(F32)
        coef = jnp.sum(da * wide, -1, keepdims=True) * (scale * scale * scale) * (-1.0 / d)
        dh[r, :] = dh[r, :] + (da * scale + wide * coef).astype(BF16)

        @pl.when(q < 3)
        def _():
            state(q + 1).start()

        @pl.when(q == 3)
        def _():
            fetch(3 * NK).start()
            down(0).start()
            for one in range(2):
                saved(0, one).start()

    def back_to_hidden(k):
        down(k).wait()

        def tile(j, _):
            q = 4 * k + j
            for one in range(2):
                saved(q, one).wait()

            @pl.when(q < 4 * NK - 1)
            def _():
                for one in range(2):
                    saved(q + 1, one).start()
            r = pl.ds(pl.multiple_of(j * quarter, quarter), quarter)
            for p in range(NK):
                part = slice(p * (cw // NK), (p + 1) * (cw // NK))
                dp = dot_t(dh[r, :], wdb[part, :]).astype(BF16).astype(F32)
                inb[0, r, part], inb[1, r, part], _ = swiglu_back(dp, gub[lax.rem(q, 2), 0, :, part], gub[lax.rem(q, 2), 1, :, part])
            return 0
        lax.fori_loop(0, 4, tile, 0)

        @pl.when(k < NK - 1)
        def _():
            down(k + 1).start()

    def compute(item, _):
        first, last = item < 3 * NK, item >= 3 * NK + 4

        @pl.when(first | last)
        def _():
            chunk(jnp.where(first, item, item - 4))

        @pl.when((item >= 3 * NK) & (item < 3 * NK + 4))
        def _():
            back_through_norm(item - 3 * NK)
        return 0

    def chunk(c):
        k, slot = lax.rem(c, NK), lax.rem(c, 2)
        wide_kind = (c < 2 * NK) | (c >= 4 * NK)

        @pl.when(c == 0)
        def _():
            at_load[0].wait()
            dy_load.start()

        @pl.when(c == 1)
        def _():
            for one in w1_load:
                one.start()

        @pl.when(c == 2 * NK)
        def _():
            dy_load.wait()
            at_load[1].start()

        @pl.when(c == 4 * NK)
        def _():
            at_load[1].wait()

        @pl.when(c < 4 * NK)
        def _():
            fetch(c).wait()

        @pl.when((c + 1 < 4 * NK) & (c + 1 != 3 * NK))
        def _():
            fetch(c + 1).start()

        @pl.when((c >= 4 * NK) & (slot == 0))
        def _():
            back_to_hidden(lax.div(c - 4 * NK, 2))

        @pl.when(wide_kind)
        def _():
            out = dot(at[...], inb[slot]).astype(BF16)
            for b in range(n):
                for i in range(cw // 128):
                    st[place(lax.rem(core + b, 2), c), b // 2, i * rg:(i + 1) * rg, :] = out[b * rg:(b + 1) * rg, i * 128:(i + 1) * 128]

        @pl.when((c >= 2 * NK) & (c < 4 * NK))
        def _():
            def sub(j, _):
                wide = cw // 2
                out = lax.dot_general(inb[slot, :, pl.ds(pl.multiple_of(j * wide, 128), wide)], dh[...], TN, preferred_element_type=F32).astype(BF16)
                for i in range(wide // rk):
                    q = (2 * k + j) * (wide // rk) + i
                    b, part = lax.div(q, NK), lax.rem(q, NK)
                    for tile in range(d // 128):
                        st[place(lax.rem(core + b, 2), c - k + part), lax.div(b, 2), tile * rk:(tile + 1) * rk, :] = \
                            out[i * rk:(i + 1) * rk, tile * 128:(tile + 1) * 128]
                return 0
            lax.fori_loop(0, 2, sub, 0)

    def exchange(c):
        return remote(st.at[place(1, c)], re.at[lax.rem(c, slots)], e_s.at[lax.rem(c, PENDING)], e_r.at[c], partner)

    def first(c):
        r, q, v = lax.rem(c, PENDING), lax.rem(c, PENDING), lax.rem(c, slots)
        return (remote(sb.at[r, 0], rt.at[v, 0], r1_s.at[q, 0], r1_r.at[c, 0], left),
                remote(sb.at[r, 1], rt.at[v, 1], r1_s.at[q, 1], r1_r.at[c, 1], right),
                remote(sb.at[r, 2], rf.at[v, 0, B], r1_s.at[q, 2], r1_r.at[c, 2], left),
                remote(sb.at[r, 3], rf.at[v, 1, A], r1_s.at[q, 3], r1_r.at[c, 3], right))

    def second(c):
        r, q, v = lax.rem(c, PENDING), lax.rem(c, PENDING), lax.rem(c, slots)
        return (remote(cb.at[r, 0], rf.at[v, 0, A], r2_s.at[q, 0], r2_r.at[c, 0], left),
                remote(cb.at[r, 1], rf.at[v, 1, B], r2_s.at[q, 1], r2_r.at[c, 1], right))

    def keep(c):
        return pltpu.make_async_copy(gout.at[lax.rem(c, 2)], g_ref.at[c], g_sem.at[lax.rem(c, 2)])

    def pair(c, to, part):
        return st[place(0, c), to, part, :].astype(F32) + re[lax.rem(c, slots), to, part, :].astype(F32)

    def step(s, _):
        def done(u):
            return sum(jnp.where(u >= at_, 1, 0) for at_ in WHEN)

        def sent(u):
            return sum(jnp.where(u >= at_, 1, 0) for at_ in SEND)

        def each(lag):
            def run(stage):
                def one(c, _):
                    stage(c)
                    return 0
                lax.fori_loop(sent(s - lag - 1), sent(s - lag), one, 0)
            return run

        lax.fori_loop(jnp.where(s == 0, 0, done(s - 1)), done(s), compute, 0)

        @each(L1)
        def _(c):
            exchange(c).wait()
            r = lax.rem(c, PENDING)
            sb[r, 0] = pair(c, far, A).astype(BF16)
            sb[r, 1] = pair(c, far, B).astype(BF16)
            sb[r, 2] = pair(c, prv, B).astype(BF16)
            sb[r, 3] = pair(c, nxt, A).astype(BF16)

        @each(L2)
        def _(c):
            for i, one in enumerate(first(c)):
                one.wait_send()
                if i < 2:
                    one.wait_recv()
            r = lax.rem(c, PENDING)
            cb[r, 0] = (pair(c, prv, A) + rt[lax.rem(c, slots), 0].astype(F32)).astype(BF16)
            cb[r, 1] = (pair(c, nxt, B) + rt[lax.rem(c, slots), 1].astype(F32)).astype(BF16)

        @each(0)
        def _(c):

            @pl.when(c >= slots)
            def _():
                pl.semaphore_wait(free.at[0], 1)
            exchange(c).start()

        @each(L2)
        def _(c):
            for one in second(c):
                one.start()

        @each(L1)
        def _(c):

            @pl.when(c >= slots)
            def _():
                pl.semaphore_wait(free.at[1], 1)
                pl.semaphore_wait(free.at[2], 1)
            for one in first(c):
                one.start()

        @each(L3)
        def _(c):
            for one in first(c)[2:]:
                one.wait_recv()
            for one in second(c):
                one.wait()
            g = (pair(c, chip, pl.ds(0, rows)) + rf[lax.rem(c, slots), 0].astype(F32) + rf[lax.rem(c, slots), 1].astype(F32)).astype(BF16)
            @pl.when(c >= 2)
            def _():
                keep(c - 2).wait()
            gout[lax.rem(c, 2)] = g
            keep(c).start()
            wide = g.astype(F32)
            ss[...] += jnp.sum((wide * wide).reshape(rows // 8, 8, 128), 0)

            @pl.when(c < chunks - slots)
            def _():
                for i, to in enumerate((partner, right, left)):
                    pl.semaphore_signal(free.at[i], inc=1, device_id={"dp": to}, device_id_type=pl.DeviceIdType.MESH)
        return 0

    lax.fori_loop(0, SEND[-1] + 1 + L3, step, 0)
    for c in (chunks - 2, chunks - 1):
        keep(c).wait()
    tell = [remote(ss, ssr.at[o], x_s.at[o], x_r.at[o], lax.rem(me + o, n)) for o in range(1, n)]
    for one in tell:
        one.start()
    total = ss[...]
    for o, one in enumerate(tell, 1):
        one.wait()
        total = total + ssr[o]
    ss_ref[...] = total

def grads(n, s, gu, at, h, dy, wg, wu, wd):
    t, d = h.shape
    ff = wg.shape[2]
    chunks, rows = 6 * NK, ff // NK // 128 * (d // n)
    assert rows == d // 128 * (ff // n // NK)
    half, slots, dma = rows // 2, chunks // 2, pltpu.SemaphoreType.DMA
    hbm = lambda a: pltpu.with_memory_space_constraint(a, pltpu.HBM)
    return pl.pallas_call(
        functools.partial(grads_kernel, n),
        in_specs=[pl.BlockSpec(memory_space=pltpu.HBM)] * 8,
        out_specs=[pl.BlockSpec(memory_space=pltpu.HBM), pl.BlockSpec(memory_space=pltpu.VMEM)],
        out_shape=[pltpu.HBM((chunks, rows, 128), BF16), pltpu.VMEM((8, 128), F32)],
        scratch_shapes=[pltpu.VMEM((d, t), BF16), pltpu.VMEM((t, d), BF16), pltpu.VMEM((2, t, ff // NK), BF16),
                        pltpu.VMEM((2, d, ff), BF16), pltpu.VMEM((ff // NK, d), BF16), pltpu.VMEM((2, 2, t // 4, ff // NK), F32),
                        pltpu.VMEM((t // 4, d), BF16), pltpu.VMEM((2, rows, 128), BF16),
                        pltpu.VMEM((RING + AHEAD, n // 2, rows, 128), BF16), pltpu.VMEM((slots, n // 2, rows, 128), BF16),
                        pltpu.VMEM((PENDING, 4, half, 128), BF16), pltpu.VMEM((slots, 2, half, 128), BF16),
                        pltpu.VMEM((PENDING, 2, half, 128), BF16), pltpu.VMEM((slots, 2, rows, 128), BF16),
                        pltpu.VMEM((8, 128), F32), pltpu.VMEM((n, 8, 128), F32),
                        dma((2,)), dma((3,)), dma((2, 2)), dma((3, 3)), dma((2,)), dma((PENDING,)), dma((chunks,)), dma((PENDING, 4)), dma((chunks, 4)),
                        dma((PENDING, 2)), dma((chunks, 2)), dma((n,)), dma((n,)), pltpu.SemaphoreType.REGULAR((3,))],
        compiler_params=pltpu.CompilerParams(vmem_limit_bytes=60 << 20, collective_id=0, has_side_effects=True),
        name="grads",
    )(*(hbm(a) for a in (s, gu, at, h, dy, wg, wu, wd)))


def update_kernel(n, count, ss_ref, g_hbm, *refs):
    given, outs, (g_ref, in_sem, g_sem, s_sem, r_sem) = refs[:9], refs[9:18], refs[18:]
    me = lax.axis_index("dp")
    chips = n // 2
    core, chip = lax.rem(me, 2), lax.div(me, 2)
    owner = lambda c, q=None: lax.rem(c + chips, chips) * 2 + (core if q is None else q)
    right, left, partner = owner(chip + 1), owner(chip - 1), owner(chip, 1 - core)
    pieces = [(i, l) for i in range(3) for l in range(2)]

    def rows_of(i, b, k=0, part=1):
        rows = outs[3 + i].shape[1]
        return pl.ds(pl.multiple_of(b * rows + k * (rows // part), 16), rows // part)

    def place(i, l, b):
        return outs[i].at[l, rows_of(i, b), :]

    def chunk_of(i, l, k):
        return i * NK + k if l else 3 * NK + k if i == 2 else 4 * NK + 2 * k + i

    def arrive(p):
        i, l = pieces[p]
        return (pltpu.make_async_copy(given[i].at[l, rows_of(i, me), :], place(i, l, me), in_sem.at[0, p]),
                pltpu.make_async_copy(given[3 + i].at[l], outs[3 + i].at[l], in_sem.at[1, p]),
                pltpu.make_async_copy(given[6 + i].at[l], outs[6 + i].at[l], in_sem.at[2, p]),
                *(pltpu.make_async_copy(g_hbm.at[chunk_of(i, l, k)], g_ref.at[chunk_of(i, l, k)], g_sem.at[p, k]) for k in range(NK)))
    for p in range(2):
        for one in arrive(p):
            one.start()
    barrier = pltpu.get_barrier_semaphore()
    for to in (left, right, partner):
        pl.semaphore_signal(barrier, inc=1, device_id={"dp": to}, device_id_type=pl.DeviceIdType.MESH)
    total = jnp.sum(ss_ref[...], keepdims=True)
    factor = jnp.minimum(1.0, 0.5 * lax.rsqrt(total / count + 1e-30))

    def renew(p):
        i, l = pieces[p]
        for one in arrive(p):
            one.wait()
        if p + 2 < len(pieces):
            for one in arrive(p + 2):
                one.start()
        full, cols = outs[3 + i].shape[1:]
        rows, tiles = (full, cols // NK // 128) if i < 2 else (full // NK, cols // 128)

        def part(k, _):
            for t in range(tiles):
                if i < 2:
                    r, own = pl.ds(0, full), rows_of(i, me)
                    c = pl.ds(pl.multiple_of(k * (cols // NK) + t * 128, 128), 128)
                else:
                    r, own = pl.ds(pl.multiple_of(k * rows, 16), rows), rows_of(i, me, k, NK)
                    c = pl.ds(t * 128, 128)
                g = g_ref[chunk_of(i, l, k), t * rows:(t + 1) * rows, :].astype(F32) * factor
                m = 0.9 * outs[3 + i][l, r, c] + 0.1 * g
                v = 0.95 * outs[6 + i][l, r, c] + 0.05 * g * g
                w = outs[i][l, own, c].astype(F32)
                outs[i][l, own, c] = (w - 0.02 * (m * lax.rsqrt(v + 1e-8) + 0.1 * w)).astype(BF16)
                outs[3 + i][l, r, c] = m
                outs[6 + i][l, r, c] = v
            return 0
        lax.fori_loop(0, NK, part, 0)

    def copy(kind, p):
        i, l = pieces[p]
        if kind == 0:
            to, b = right, me
        elif kind == 1:
            to, b = left, me
        elif kind == 2:
            to, b = (right, owner(chip - 1)) if l == 0 else (left, owner(chip + 1))
        else:
            to = partner
            b = (me, owner(chip - 1), owner(chip + 1), owner(chip + 2))[kind - 3]
        ref = place(i, l, b)
        return pltpu.make_async_remote_copy(src_ref=ref, dst_ref=ref, send_sem=s_sem.at[kind, p], recv_sem=r_sem.at[kind, p],
                                            device_id={"dp": to}, device_id_type=pl.DeviceIdType.MESH)
    zero, one_ = [p for p, (i, l) in enumerate(pieces) if l == 0], [p for p, (i, l) in enumerate(pieces) if l == 1]
    for p in range(len(pieces)):
        renew(p)
        if p == 0:
            pl.semaphore_wait(barrier, 3)
        if p > 0:
            copy(0 if pieces[p - 1][1] == 0 else 1, p - 1).start()
    copy(1, len(pieces) - 1).start()
    for a, b in zip(zero, one_):
        copy(0, b).start()
        copy(1, a).start()
    for p in range(len(pieces)):
        copy(3, p).start()
    for a, b in zip(zero, one_):
        copy(0, a).wait_recv()
        copy(2, a).start()
        copy(4, a).start()
        copy(1, b).wait_recv()
        copy(2, b).start()
        copy(5, b).start()
    for a, b in zip(one_, zero):
        copy(0, a).wait_recv()
        copy(4, a).start()
        copy(1, b).wait_recv()
        copy(5, b).start()
    for a, b in zip(zero, one_):
        for p in (a, b):
            copy(2, p).wait_recv()
            copy(6, p).start()
    for p in range(len(pieces)):
        for kind in range(7):
            copy(kind, p).wait_send()
            if kind >= 3:
                copy(kind, p).wait_recv()

def update(n, ss, g, ws, ms, vs):
    dma, vmem = pltpu.SemaphoreType.DMA, pl.BlockSpec(memory_space=pltpu.VMEM)
    count = n * sum(m.size for m in ms)
    out = pl.pallas_call(
        functools.partial(update_kernel, n, count),
        in_specs=[vmem] + [pl.BlockSpec(memory_space=pltpu.HBM)] * 10,
        out_specs=[vmem] * 9,
        out_shape=[pltpu.VMEM(a.shape, a.dtype) for a in (*ws, *ms, *vs)],
        scratch_shapes=[pltpu.VMEM(g.shape, BF16), dma((3, 6)), dma((6, NK)), dma((7, 6)), dma((7, 6))],
        compiler_params=pltpu.CompilerParams(vmem_limit_bytes=8 << 20, collective_id=1, has_side_effects=True),
        name="update",
    )(ss, *(pltpu.with_memory_space_constraint(a, pltpu.HBM) for a in (g, *ws, *ms, *vs)))
    return out

def store_kernel(*refs):
    half = (len(refs) - 1) // 2
    copies = [pltpu.make_async_copy(refs[i], refs[half + i], refs[-1].at[i]) for i in range(half)]
    for one in copies:
        one.start()
    for one in copies:
        one.wait()

def store(arrays):
    k = len(arrays)
    return pl.pallas_call(
        store_kernel, in_specs=[pl.BlockSpec(memory_space=pltpu.VMEM)] * k, out_specs=[pl.BlockSpec(memory_space=pltpu.HBM)] * k,
        out_shape=[pltpu.HBM(a.shape, a.dtype) for a in arrays], scratch_shapes=[pltpu.SemaphoreType.DMA((k,))],
        compiler_params=pltpu.CompilerParams(vmem_limit_bytes=1 << 20), name="store")(*arrays)

def solution(mesh):
    n = mesh.shape["dp"]

    def step(x, dy, wg, wu, wd, mg, mu, md, vg, vu, vd):
        s, gu, at, h = tokens(x, dy, wg, wu, wd)
        g, ss = grads(n, s, gu, at, h, dy, wg, wu, wd)
        return tuple(store(update(n, ss, g, (wg, wu, wd), (mg, mu, md), (vg, vu, vd))))

    data, whole, rows = P(("rep", "dp"), None, None), P(None, None, None), P(None, "dp", None)
    return jax.shard_map(step, mesh=mesh, in_specs=(data,) * 2 + (whole,) * 3 + (rows,) * 6,
                         out_specs=(P("rep", None, None),) * 3 + (P("rep", "dp", None),) * 6, check_vma=False)
```
